256 devices in a mesh: dp: 8 (over x_lo, y), mp: 32 (over z, x_hi, core).
Axes of the slice: x: 4 (x_hi: 2, x_lo: 2; x = x_hi * 2 + x_lo), y: 4, z: 8, core: 2. Of those that a mesh axis runs over, the one named last changes fastest.
Arguments:
- tokens: bfloat16 [1024, 6144], P(('dp', 'mp')), may hold values from -6 to 6
- norm_gain: float32 [6144], replicated, may hold values from 0.5 to 1.5
- w_query: bfloat16 [6144, 4096], P('dp', 'mp'), as said below
- w_key: bfloat16 [6144, 4096], P('dp', 'mp'), as said below
- w_value: bfloat16 [6144, 4096], P('dp', 'mp'), may hold values from -0.078125 to 0.078125
- w_inner: bfloat16 [6144, 24576], P('dp', 'mp'), may hold values from -0.078125 to 0.078125
- bias_inner: float32 [24576], P('mp'), may hold values from -3 to 3
- w_attn_out: bfloat16 [4096, 6144], P('mp', 'dp'), may hold values from -0.09375 to 0.09375
- w_outer: bfloat16 [24576, 6144], P('mp', 'dp'), may hold values from -0.0390625 to 0.0390625
- temper: float32 [32], P('mp'), may hold values from 0.5 to 24
Outputs:
- result: bfloat16 [1024, 6144], P(('dp', 'mp'))
The draws below stay inside these ranges and needn't reach their ends.
Inputs may be any that keep to these rules, and one draw needn't show every extreme that they name: `w_query`: entries of order 6144 ** -0.5. `w_key`: entries of order 6144 ** -0.5.
All inputs are finite; a program needn't handle non-finite values.
Results may differ from the reference program's by a relative error of at most 0.023.
Values may be sent and summed in bfloat16 or wider, within the bound.
A program may use at most 64 MiB of HBM per device.

```python
import math
import jax
import jax.numpy as jnp
from jax import lax

D = 6144
HEADS = 32
HEAD = 128
FF = 24576
HD = 4096
PATCHES = 128
TOKENS = 1024
N_DP = 8


def shared_draws(key):
    key_query = jax.random.fold_in(key, 11)
    key_noise = jax.random.fold_in(key, 12)
    key_temper = jax.random.fold_in(key, 14)
    scale = D ** (-0.5)
    limit = 6.0 * scale
    query = jnp.clip(jax.random.normal(key_query, (D, HD), jnp.float32) * scale, -limit, limit)
    noise = jnp.clip(jax.random.normal(key_noise, (D, HD), jnp.float32) * scale, -limit, limit)
    temper = jnp.exp(jax.random.uniform(key_temper, (HEADS,), jnp.float32, jnp.log(0.5), jnp.log(6.0)))
    keys = noise
    return (query, keys, temper)


def draw_w_query(key, part):
    return shared_draws(key)[0].astype(jnp.bfloat16)


def draw_w_key(key, part):
    return shared_draws(key)[1].astype(jnp.bfloat16)


def draw_temper(key, part):
    return shared_draws(key)[2]


def level_of(rng, extent, split, low, high):
    level, own = 1.0, jax.random.fold_in(rng, 6)
    for dim, blocks in split:
        heights = jnp.exp(jax.random.uniform(jax.random.fold_in(own, dim), (blocks,), jnp.float32, low / len(split), high / len(split)))
        level = level * jnp.repeat(heights, extent[dim] // blocks).reshape([-1 if axis == dim else 1 for axis in range(len(extent))])
    return level


def bell_draw(stream_key, extent, deviation, most, shards=(), kind=jnp.bfloat16):
    result = deviation * jax.random.normal(stream_key, extent, jnp.float32)
    if shards:
        result = result * level_of(stream_key, extent, shards, -0.22, 0.18)
    return jnp.clip(result, -most, most).astype(kind)


def setup_inputs(seed: int = 0) -> dict:
    streams_of = jax.random.split(jax.random.key(seed), 11)
    return {
        "tokens": bell_draw(streams_of[0], (TOKENS, D), 1.0, 6.0, ((0, 256),)),
        "norm_gain": jnp.clip(1.0 + 0.1 * jax.random.normal(streams_of[1], (D,), jnp.float32), 0.5, 1.5),
        "w_query": draw_w_query(jax.random.fold_in(streams_of[10], 71), 0),
        "w_key": draw_w_key(jax.random.fold_in(streams_of[10], 71), 0),
        "w_value": bell_draw(streams_of[4], (D, HD), D ** -0.5, 0.078125, ((0, 8), (1, 32))),
        "w_inner": bell_draw(streams_of[5], (D, FF), D ** -0.5, 0.078125, ((0, 8), (1, 32))),
        "bias_inner": bell_draw(streams_of[6], (FF,), 0.5, 3.0, ((0, 32),), jnp.float32),
        "w_attn_out": bell_draw(streams_of[7], (HD, D), HD ** -0.5, 0.09375, ((0, 32), (1, 8))),
        "w_outer": bell_draw(streams_of[8], (FF, D), FF ** -0.5, 0.0390625, ((0, 32), (1, 8))),
        "temper": draw_temper(jax.random.fold_in(streams_of[10], 71), 0),
    }


def normalize(values):
    center = values - lax.optimization_barrier(jnp.mean(values, axis=-1, keepdims=True))
    spread = lax.optimization_barrier(jnp.mean(center * center, axis=-1, keepdims=True))
    return center * lax.rsqrt(spread + 1e-06)

def reference(tokens, norm_gain, w_query, w_key, w_value, w_inner, bias_inner, w_attn_out, w_outer, temper):
    local = tokens.astype(jnp.float32)
    normed = (normalize(local) * norm_gain.astype(jnp.float32)).astype(jnp.bfloat16)
    query = jnp.dot(normed, w_query, preferred_element_type=jnp.float32).astype(jnp.bfloat16)
    keys = jnp.dot(normed, w_key, preferred_element_type=jnp.float32).astype(jnp.bfloat16)
    values = jnp.dot(normed, w_value, preferred_element_type=jnp.float32).astype(jnp.bfloat16)
    shape = (N_DP, PATCHES, HEADS, HEAD)
    query_norm = normalize(query.astype(jnp.float32).reshape(shape)).astype(jnp.bfloat16)
    key_norm = normalize(keys.astype(jnp.float32).reshape(shape)).astype(jnp.bfloat16)
    values4 = values.reshape(shape).astype(jnp.float32)
    scale = temper.astype(jnp.float32) / math.sqrt(HEAD)
    scores = jnp.einsum('bqhc,bkhc->bhqk', query_norm.astype(jnp.float32), key_norm.astype(jnp.float32))
    scores = scores * scale[None, :, None, None]
    probs = jax.nn.softmax(scores, axis=-1).astype(jnp.bfloat16)
    mixed = jnp.einsum('bhqk,bkhc->bqhc', probs.astype(jnp.float32), values4)
    mixed = mixed.astype(jnp.bfloat16).reshape(TOKENS, HD)
    inner = jnp.dot(normed, w_inner, preferred_element_type=jnp.float32) + bias_inner.astype(jnp.float32)
    activ = jax.nn.gelu(inner, approximate=False).astype(jnp.bfloat16)
    total = jnp.dot(mixed, w_attn_out, preferred_element_type=jnp.float32)
    total = total + jnp.dot(activ, w_outer, preferred_element_type=jnp.float32)
    return (local + total).astype(jnp.bfloat16)
```

```python
import functools
import math

import jax
import jax.numpy as jnp
from jax import lax
from jax.experimental import pallas as pl
from jax.experimental.pallas import tpu as pltpu
from jax.sharding import PartitionSpec as P

HEAD = 128
NX, NY, NZ = 2, 4, 8
MESH = pl.DeviceIdType.MESH
F32, BF16 = jnp.float32, jnp.bfloat16


def normalize(values):
    center = values - jnp.mean(values, axis=-1, keepdims=True)
    spread = jnp.mean(center * center, axis=-1, keepdims=True)
    return center * lax.rsqrt(spread + 1e-06)


def wait_bytes(ref, sem):
    pltpu.make_async_copy(ref, ref, sem).wait()


def block_kernel(
    tokens, gain, bias, temper, w_query, w_key, w_value, w_inner, w_attn, w_outer,
    out,
    w_qkv, w_in, w_at, w_out, nsend, nrecv, stage, xg, pf, asend, arecv, brsend, brrecv,
    blsend, blrecv, sf, csend, crecv, qkv, ag, mg, og, esend, erecv, rsend, rrecv, fsend, frecv,
    win_sem, n_send, n_recv, m_send, m_recv, r_send, r_recv, s_send, s_recv,
    a_send, ar_recv, al_recv, b_send, br_recv, bl_recv, c_send, c_recv,
    gx_send, gx_recv, gy_send, gr_recv, gl_recv, h_send, hr_recv, hl_recv,
    e_send, e_recv, z_send, z_recv, f_send, f_recv,
):
    rows, depth = nsend.shape[1:]
    wide = w_qkv.shape[1]
    full = pf.shape[3]
    cut = 5 * HEAD
    half = depth // 2
    i, j = lax.axis_index("dp"), lax.axis_index("mp")
    xl, y = i // NY, lax.rem(i, NY)
    z, xh, c = j // 4, lax.rem(j // 2, 2), lax.rem(j, 2)
    yr, yl, y2 = lax.rem(y + 1, NY), lax.rem(y + NY - 1, NY), lax.rem(y + 2, NY)
    zr, zl = lax.rem(z + 1, NZ), lax.rem(z + NZ - 1, NZ)
    sibling = (i, z * 4 + xh * 2 + 1 - c)
    partner = ((1 - xl) * NY + y, j)
    y_right, y_left = (xl * NY + yr, j), (xl * NY + yl, j)
    z_right, z_left = (i, zr * 4 + xh * 2 + c), (i, zl * 4 + xh * 2 + c)

    def send(src, dst, send_sem, recv_sem, target):
        pltpu.make_async_remote_copy(
            src_ref=src, dst_ref=dst, send_sem=send_sem, recv_sem=recv_sem,
            device_id=target, device_id_type=MESH,
        ).start()

    barrier = pltpu.get_barrier_semaphore()
    n_plane = 4 * NX * NY
    here = i * 4 + xh * 2 + c

    def greet(d, carry):
        t = lax.rem(here + d, n_plane)
        pl.semaphore_signal(
            barrier, inc=1, device_id=(t // 4, z * 4 + lax.rem(t, 4)), device_id_type=MESH
        )
        return carry

    lax.fori_loop(1, n_plane, greet, 0)
    for target in (z_right, z_left):
        pl.semaphore_signal(barrier, inc=1, device_id=target, device_id_type=MESH)

    loads = [
        pltpu.make_async_copy(w, w_qkv.at[:, n * HEAD : (n + 1) * HEAD], win_sem.at[n])
        for n, w in enumerate((w_query, w_key, w_value))
    ]
    loads.append(pltpu.make_async_copy(w_inner, w_in, win_sem.at[3]))
    loads.append(pltpu.make_async_copy(w_attn, w_at, win_sem.at[4]))
    loads.append(pltpu.make_async_copy(w_outer, w_out, win_sem.at[5]))
    for load in loads:
        load.start()

    normed = (normalize(tokens[...].astype(F32)) * gain[...]).astype(BF16)
    for p in range(NX * NY):
        nsend[p] = normed[:, p * depth : (p + 1) * depth]
    lane = i * 2 + xh
    nrecv[c, lane] = nsend[i]
    pl.semaphore_wait(barrier, n_plane + 1)

    n_lane = 2 * NX * NY

    def scatter_normed(d, carry):
        t = lax.rem(lane + d, n_lane)
        send(
            nsend.at[t // 2], nrecv.at[c, lane], n_send, n_recv,
            (t // 2, z * 4 + lax.rem(t, 2) * 2 + c),
        )
        return carry

    lax.fori_loop(1, n_lane, scatter_normed, 0)
    wait_bytes(nrecv.at[0, pl.ds(0, n_lane - 1)], n_recv)
    send(nrecv.at[c], nrecv.at[c], m_send, m_recv, sibling)
    wait_bytes(nrecv.at[0], m_recv)
    for q in range(NX * NY):
        p = q % NX * NY + q // NX
        for s in range(4):
            at = q * 4 * rows + s * rows
            stage[at : at + rows, :] = nrecv[s % 2, p * 2 + s // 2].astype(F32)
    xg[0] = stage[...].astype(BF16).reshape(xg.shape[1:])

    def ring_right(src, dst):
        send(xg.at[src, c], xg.at[dst, c], r_send, r_recv.at[dst], z_right)

    def ring_left(src, dst):
        send(xg.at[src, c], xg.at[dst, c], r_send, r_recv.at[dst], z_left)

    def ring(d):
        top, low = pl.ds(0, 8 * rows), pl.ds(8 * rows, 8 * rows)
        if d == 0:
            ring_right(0, 7)
            ring_left(0, 1)
            return
        if d == 4:
            wait_bytes(xg.at[4, 0, top], r_recv.at[4])
            wait_bytes(xg.at[4, 0, low], r_recv.at[8])
            send(xg.at[4, c], xg.at[4, c], s_send, s_recv.at[4], sibling)
            return
        wait_bytes(xg.at[8 - d, 0], r_recv.at[8 - d])
        if d < 3:
            ring_right(8 - d, 7 - d)
        else:
            send(xg.at[5, c, top], xg.at[4, c, top], r_send, r_recv.at[4], z_right)
        send(xg.at[8 - d, c], xg.at[8 - d, c], s_send, s_recv.at[8 - d], sibling)
        wait_bytes(xg.at[d, 0], r_recv.at[d])
        if d < 3:
            ring_left(d, d + 1)
        else:
            send(xg.at[3, c, low], xg.at[4, c, low], r_send, r_recv.at[8], z_left)
        send(xg.at[d, c], xg.at[d, c], s_send, s_recv.at[d], sibling)

    units = [(0,), (7, 1), (6, 2), (5, 3), (4,)]

    def project(k):
        if k != 0:
            wait_bytes(xg.at[k, 0], s_recv.at[k])
        x = xg[k].reshape(32 * rows, depth)
        pf[k, :, :, :wide] = jnp.dot(
            x, w_qkv[...], preferred_element_type=F32
        ).reshape(NY, 8 * rows, wide)
        pf[k, :, :, wide:] = jnp.dot(
            x, w_in[...], preferred_element_type=F32
        ).reshape(NY, 8 * rows, full - wide)

    def stage_a(k):
        asend[k] = pf[k, y2].astype(BF16)
        right, left = pl.ds(0, cut), pl.ds(cut, full - cut)
        send(asend.at[k, :, right], arecv.at[k, :, right], a_send, ar_recv.at[k], y_right)
        send(asend.at[k, :, left], arecv.at[k, :, left], a_send, al_recv.at[k], y_left)

    def stage_b(k):
        wait_bytes(arecv.at[k, :, pl.ds(0, cut)], ar_recv.at[k])
        brsend[k, :, :cut] = (pf[k, yr, :, :cut] + arecv[k, :, :cut].astype(F32)).astype(BF16)
        brsend[k, :, cut:] = pf[k, yr, :, cut:].astype(BF16)
        send(brsend.at[k], brrecv.at[k], b_send, br_recv.at[k], y_right)
        wait_bytes(arecv.at[k, :, pl.ds(cut, full - cut)], al_recv.at[k])
        blsend[k, :, :cut] = pf[k, yl, :, :cut].astype(BF16)
        blsend[k, :, cut:] = (pf[k, yl, :, cut:] + arecv[k, :, cut:].astype(F32)).astype(BF16)
        send(blsend.at[k], blrecv.at[k], b_send, bl_recv.at[k], y_left)

    def stage_c(k):
        wait_bytes(brrecv.at[k], br_recv.at[k])
        wait_bytes(blrecv.at[k], bl_recv.at[k])
        total = pf[k, y] + brrecv[k].astype(F32) + blrecv[k].astype(F32)
        low, high = total[: 4 * rows], total[4 * rows :]
        csend[k] = jnp.where(xl == 0, high, low).astype(BF16)
        send(csend.at[k], crecv.at[k], c_send, c_recv.at[k], partner)
        sf[k] = jnp.where(xl == 0, low, high)

    def stage_d(k):
        wait_bytes(crecv.at[k], c_recv.at[k])
        total = sf[k] + crecv[k].astype(F32)
        qkv[k] = total[:, :wide].astype(BF16)
        inner = total[:, wide:] + bias[...]
        activ = 0.5 * inner * (1.0 + lax.erf(inner * math.sqrt(0.5)))
        ag[k, y, xl] = activ.astype(BF16)
        send(ag.at[k, y, xl], ag.at[k, y, xl], gx_send, gx_recv.at[k], partner)

    def gather_y(g, k, at):
        wait_bytes(g.at[at + (0, 0)], gx_recv.at[k])
        send(g.at[at + (y,)], g.at[at + (y,)], gy_send, gr_recv.at[k], y_right)
        send(g.at[at + (y,)], g.at[at + (y,)], gy_send, gl_recv.at[k], y_left)

    def gather_far(g, k, at):
        wait_bytes(g.at[at + (0,)], gr_recv.at[k])
        send(g.at[at + (yl, 0)], g.at[at + (yl, 0)], h_send, hr_recv.at[k], y_right)
        wait_bytes(g.at[at + (0,)], gl_recv.at[k])
        send(g.at[at + (yr, 1)], g.at[at + (yr, 1)], h_send, hl_recv.at[k], y_left)

    def gather_done(g, k, at):
        wait_bytes(g.at[at + (0, 0)], hr_recv.at[k])
        wait_bytes(g.at[at + (0, 0)], hl_recv.at[k])

    def each(stage_fn, u):
        if 0 <= u < len(units):
            for k in units[u]:
                stage_fn(k)

    def attend():
        query = qkv[:, :, :HEAD].reshape(32 * rows, HEAD)
        key = qkv[:, :, HEAD : 2 * HEAD].reshape(32 * rows, HEAD)
        value = qkv[:, :, 2 * HEAD :].reshape(32 * rows, HEAD)
        query_norm = normalize(query.astype(F32)).astype(BF16)
        key_norm = normalize(key.astype(F32)).astype(BF16)
        scores = lax.dot_general(
            query_norm, key_norm, (((1,), (1,)), ((), ())), preferred_element_type=F32
        )
        scores = scores * (temper[0] * (1.0 / math.sqrt(HEAD)))
        weight = jnp.exp(scores - jnp.max(scores, axis=-1, keepdims=True))
        probs = (weight / jnp.sum(weight, axis=-1, keepdims=True)).astype(BF16)
        mg[y, xl] = jnp.dot(probs, value, preferred_element_type=F32).astype(BF16)
        send(mg.at[y, xl], mg.at[y, xl], gx_send, gx_recv.at[8], partner)

    ring(0)
    for load in loads[:4]:
        load.wait()
    for u in range(len(units) + 6):
        if 1 <= u <= 4:
            ring(u)
        each(stage_b, u - 1)
        each(stage_c, u - 2)
        each(stage_d, u - 3)
        if u - 3 == 4:
            attend()
        each(lambda k: gather_y(ag, k, (k,)), u - 4)
        if u - 4 == 4:
            gather_y(mg, 8, ())
        each(lambda k: gather_far(ag, k, (k,)), u - 5)
        if u - 5 == 4:
            gather_far(mg, 8, ())
        if u < 5:
            each(project, u)
            each(stage_a, u)

    for load in loads[4:]:
        load.wait()
    gather_done(mg, 8, ())

    def project_out(k):
        gather_done(ag, k, (k,))
        hidden = ag[k].reshape(32 * rows, depth)
        mixed = mg[:, :, 4 * rows * k : 4 * rows * (k + 1), :].reshape(32 * rows, HEAD)
        total = jnp.dot(hidden, w_out[...], preferred_element_type=F32)
        total = total + jnp.dot(mixed, w_at[...], preferred_element_type=F32)
        og[k] = total.reshape(og.shape[1:])
        esend[k] = og[k, 1 - c].astype(BF16)
        send(esend.at[k], erecv.at[k], e_send, e_recv.at[k], sibling)

    def combined(k):
        wait_bytes(erecv.at[k], e_recv.at[k])
        return og[k, c] + erecv[k].astype(F32)

    low, high = pl.ds(0, half), pl.ds(half, half)

    def reduce_out(k):
        total = combined(k)
        if k == 4:
            rsend[4] = total.astype(BF16)
            send(rsend.at[4, :, low], rrecv.at[3, :, low], z_send, z_recv.at[3], z_right)
            send(rsend.at[4, :, high], rrecv.at[5, :, high], z_send, z_recv.at[5], z_left)
            return
        if k == 3:
            wait_bytes(rrecv.at[3, :, low], z_recv.at[3])
            rsend[3, :, :half] = (total[:, :half] + rrecv[3, :, :half].astype(F32)).astype(BF16)
            rsend[3, :, half:] = total[:, half:].astype(BF16)
        elif k == 5:
            wait_bytes(rrecv.at[5, :, high], z_recv.at[5])
            rsend[5, :, :half] = total[:, :half].astype(BF16)
            rsend[5, :, half:] = (total[:, half:] + rrecv[5, :, half:].astype(F32)).astype(BF16)
        else:
            wait_bytes(rrecv.at[k], z_recv.at[k])
            rsend[k] = (total + rrecv[k].astype(F32)).astype(BF16)
        to = k - 1 if k < 4 else k + 1
        send(rsend.at[k], rrecv.at[to], z_send, z_recv.at[to], z_right if k < 4 else z_left)

    order = [(4,), (5, 3), (6, 2), (7, 1), (0,)]
    for u in range(6):
        if u < 5:
            for k in order[u]:
                project_out(k)
        if u >= 1 and u < 5:
            for k in order[u - 1]:
                reduce_out(k)
    total = combined(0)
    wait_bytes(rrecv.at[0], z_recv.at[0])
    wait_bytes(rrecv.at[8], z_recv.at[8])
    total = total + rrecv[0].astype(F32) + rrecv[8].astype(F32)
    mine = c == y // 2
    for q in range(4):
        for s in range(4):
            at = q * 4 * rows + s * rows
            fsend[q * 4 + s] = total[at : at + rows].astype(BF16)
    for q in range(4):
        p = q % NX * NY + 2 * c + q // NX
        for s in range(4):
            own = jnp.logical_and(p == i, s == xh * 2 + c)

            @pl.when(own)
            def _():
                frecv[i * 2 + xh] = fsend[q * 4 + s]

            @pl.when(jnp.logical_not(own))
            def _():
                send(fsend.at[q * 4 + s], frecv.at[i * 2 + xh], f_send, f_recv, (p, z * 4 + s))

    @pl.when(mine)
    def _():
        wait_bytes(frecv.at[pl.ds(0, n_lane - 1)], f_recv)
        wait_bytes(frecv.at[pl.ds(0, n_lane - 1)], f_send)

    @pl.when(jnp.logical_not(mine))
    def _():
        wait_bytes(frecv, f_recv)
        wait_bytes(frecv, f_send)

    for p in range(NX * NY):
        cols = slice(p * depth, (p + 1) * depth)
        total = frecv[2 * p].astype(F32) + frecv[2 * p + 1].astype(F32)
        out[:, cols] = (tokens[:, cols].astype(F32) + total).astype(BF16)

    wait_bytes(nrecv.at[0, pl.ds(0, n_lane - 1)], n_send)
    wait_bytes(nrecv.at[0], m_send)
    wait_bytes(xg.at[pl.ds(0, 7), 0], r_send)
    wait_bytes(xg.at[pl.ds(0, 7), 0], s_send)
    wait_bytes(asend, a_send)
    wait_bytes(brsend, b_send)
    wait_bytes(blsend, b_send)
    wait_bytes(csend, c_send)
    wait_bytes(ag.at[:, 0, 0], gx_send)
    wait_bytes(mg.at[0, 0], gx_send)
    wait_bytes(ag.at[:, pl.ds(0, 2)], gy_send)
    wait_bytes(mg.at[pl.ds(0, 2)], gy_send)
    wait_bytes(ag.at[:, 0], h_send)
    wait_bytes(mg.at[0], h_send)
    wait_bytes(esend, e_send)
    wait_bytes(rsend.at[pl.ds(0, 7)], z_send)


def per_device(
    tokens, norm_gain, w_query, w_key, w_value, w_inner, bias_inner, w_attn_out, w_outer, temper
):
    rows, width = tokens.shape
    depth = w_query.shape[0]
    wide = 3 * HEAD
    hidden = w_inner.shape[1]
    full = wide + hidden
    vmem = pl.BlockSpec(memory_space=pltpu.VMEM)
    smem = pl.BlockSpec(memory_space=pltpu.SMEM)
    hbm = pl.BlockSpec(memory_space=pl.ANY)
    dma = pltpu.SemaphoreType.DMA
    block = 8 * rows
    return pl.pallas_call(
        block_kernel,
        out_shape=jax.ShapeDtypeStruct((rows, width), BF16),
        in_specs=[vmem, vmem, vmem, smem] + [hbm] * 6,
        out_specs=vmem,
        scratch_shapes=[
            pltpu.VMEM((depth, wide), BF16),
            pltpu.VMEM((depth, hidden), BF16),
            pltpu.VMEM((HEAD, depth), BF16),
            pltpu.VMEM((hidden, depth), BF16),
            pltpu.VMEM((8, rows, depth), BF16),
            pltpu.VMEM((2, 16, rows, depth), BF16),
            pltpu.VMEM((32 * rows, depth), F32),
            pltpu.VMEM((NZ, 2, 16 * rows, depth), BF16),
            pltpu.VMEM((NZ, NY, block, full), F32),
            pltpu.VMEM((NZ, block, full), BF16),
            pltpu.VMEM((NZ, block, full), BF16),
            pltpu.VMEM((NZ, block, full), BF16),
            pltpu.VMEM((NZ, block, full), BF16),
            pltpu.VMEM((NZ, block, full), BF16),
            pltpu.VMEM((NZ, block, full), BF16),
            pltpu.VMEM((NZ, 4 * rows, full), F32),
            pltpu.VMEM((NZ, 4 * rows, full), BF16),
            pltpu.VMEM((NZ, 4 * rows, full), BF16),
            pltpu.VMEM((NZ, 4 * rows, wide), BF16),
            pltpu.VMEM((NZ, NY, NX, 4 * rows, hidden), BF16),
            pltpu.VMEM((NY, NX, 32 * rows, HEAD), BF16),
            pltpu.VMEM((NZ, 2, 16 * rows, depth), F32),
            pltpu.VMEM((NZ, 16 * rows, depth), BF16),
            pltpu.VMEM((NZ, 16 * rows, depth), BF16),
            pltpu.VMEM((NZ, 16 * rows, depth), BF16),
            pltpu.VMEM((NZ + 1, 16 * rows, depth), BF16),
            pltpu.VMEM((16, rows, depth), BF16),
            pltpu.VMEM((16, rows, depth), BF16),
            dma((6,)), dma, dma, dma, dma, dma, dma((9,)), dma, dma((8,)),
            dma, dma((8,)), dma((8,)), dma, dma((8,)), dma((8,)), dma, dma((8,)),
            dma, dma((9,)), dma, dma((9,)), dma((9,)), dma, dma((9,)), dma((9,)),
            dma, dma((8,)), dma, dma((9,)), dma, dma,
        ],
        compiler_params=pltpu.CompilerParams(
            collective_id=0, has_side_effects=True, vmem_limit_bytes=60 * 1024 * 1024
        ),
        name="encoder_block",
    )(
        tokens, norm_gain.reshape(1, -1), bias_inner.reshape(1, -1), temper,
        w_query, w_key, w_value, w_inner, w_attn_out, w_outer,
    )


def solution(mesh):
    return jax.shard_map(
        per_device,
        mesh=mesh,
        in_specs=(
            P(("dp", "mp"), None),
            P(),
            P("dp", "mp"),
            P("dp", "mp"),
            P("dp", "mp"),
            P("dp", "mp"),
            P("mp"),
            P("mp", "dp"),
            P("mp", "dp"),
            P("mp"),
        ),
        out_specs=P(("dp", "mp"), None),
        check_vma=False,
    )
```

```python
import functools
import math

import jax
import jax.numpy as jnp
from jax import lax
from jax.experimental import pallas as pl
from jax.experimental.pallas import tpu as pltpu
from jax.sharding import PartitionSpec as P

HEAD = 128
NX, NY, NZ = 2, 4, 8
MESH = pl.DeviceIdType.MESH
F32, BF16 = jnp.float32, jnp.bfloat16
GROUPS = ((0, 384, "x"), (384, 1152, "y"))
REDUCE_AT_ONCE = ((), (5,))
REDUCE_IN_TWO = (0, 4)
GATHER_AT_ONCE = (4, 7, 8)
GATHER_IN_TWO = (1,)
Y_FIRST = (5, 6)
PEERS = tuple((dx, dy) for dy in (2, 1, 3, 0) for dx in (1, 0) if dx or dy)
SCHEDULE = (
    "r.0", "w0.0", "p0.0", "p1.0", "b.1", "r0.1", "p0.1", "r1.1", "q0.0", "b.7",
    "r0.7", "p0.7", "m0.0", "q0.7", "r1.7", "p1.1", "r0.2", "q0.1", "m0.1", "r0.6",
    "q1.0", "p1.7", "r1.2", "m0.7", "q1.7", "r1.6", "p0.2", "p1.2", "q0.2", "m0.2",
    "m1.0", "p0.6", "m1.1", "p1.6", "m0.6", "q0.6", "r0.3", "r0.5", "q1.1", "q2.7",
    "q2.0", "r1.3", "r1.5", "m1.2", "p0.3", "q0.3", "p0.5", "q0.5", "p1.5", "q1.2",
    "m0.5", "q1.6", "r.4", "q3.0", "p1.3", "m0.3", "p0.4", "p1.4", "m0.4", "q0.4",
    "q1.5", "m2.0", "m2.1", "q1.3", "m1.6", "m1.3", "q1.4", "m2.2", "q2.2", "q2.6",
    "q3.7", "y.0", "m1.4", "m1.5", "q2.1", "q2.5", "q2.3", "m3.1", "q2.4", "m1.7",
    "m2.3", "q3.2", "m2.6", "m2.4", "q3.3", "q3.6", "y.5", "q3.4", "m3.3", "q3.1",
    "q3.5", "m3.2", "m3.6", "a.0", "y.3", "y.6", "m2.7", "f.5", "g0.0", "y.2",
    "f.3", "g1.0", "w1.0", "o.4", "f.6", "f.0", "s1.4", "s0.4", "f.2", "o.5",
    "m3.7", "y.1", "o.3", "s0.5", "o.0", "s1.3", "s1.5", "s0.3", "o.6", "o.2",
    "s0.6", "s1.2", "s1.6", "s0.2", "o.7", "o.1", "s0.7", "s0.1",
)
OFFSETS = sorted(
    ((dx, dy) for dx in range(4) for dy in range(NY)),
    key=lambda o: -(min(o[0], 4 - o[0]) + min(o[1], NY - o[1])),
)

scope = jax.named_scope


def normalize(values):
    center = values - jnp.mean(values, axis=-1, keepdims=True)
    spread = jnp.mean(center * center, axis=-1, keepdims=True)
    return center * lax.rsqrt(spread + 1e-06)


def wait_bytes(ref, sem):
    pltpu.make_async_copy(ref, ref, sem).wait()


def send(src, dst, send_sem, recv_sem, target):
    pltpu.make_async_remote_copy(
        src_ref=src, dst_ref=dst, send_sem=send_sem, recv_sem=recv_sem,
        device_id=target, device_id_type=MESH,
    ).start()


def block_kernel(
    tokens_ref, gain_ref, bias_ref, temper, w_query, w_key, w_value, w_inner, w_attn, w_outer,
    out,
    tokens, gain, bias, w_qkv, w_in, w_at, w_out, nsend, nrecv, stage, xg, pf, groups,
    direct, qkv, ag, mg, og, esend, erecv, rsend, rrecv, fsend, frecv,
    in_sem, win_sem, n_send, n_recv, m_send, m_recv, r_send, r_recv, s_send, s_recv,
    gd_send, gd_recv, gx_send, gx_recv, gy_send, gr_recv, gl_recv, h_send, hr_recv, hl_recv,
    e_send, e_recv, z_send, z_recv, f_send, f_recv,
):
    rows, depth = nsend.shape[1:]
    tile = 4 * rows
    half = depth // 2
    i, j = lax.axis_index("dp"), lax.axis_index("mp")
    xl, y = i // NY, lax.rem(i, NY)
    z, xh, c = j // 4, lax.rem(j // 2, 2), lax.rem(j, 2)
    x, me = xh * 2 + xl, y * NX + xl
    yr, yl, y2 = lax.rem(y + 1, NY), lax.rem(y + NY - 1, NY), lax.rem(y + 2, NY)
    zr, zl = lax.rem(z + 1, NZ), lax.rem(z + NZ - 1, NZ)
    sibling = (i, z * 4 + xh * 2 + 1 - c)
    partner = ((1 - xl) * NY + y, j)
    y_right, y_left = (xl * NY + yr, j), (xl * NY + yl, j)
    z_right, z_left = (i, zr * 4 + xh * 2 + c), (i, zl * 4 + xh * 2 + c)

    planes = (z, zl, zr)

    def in_plane(dx, to_y, core, n=0):
        to = lax.rem(x + dx, 4)
        return (lax.rem(to, 2) * NY + to_y, planes[n] * 4 + (to // 2) * 2 + core)

    inputs = [
        pltpu.make_async_copy(src, dst, in_sem.at[n])
        for n, (src, dst) in enumerate(((tokens_ref, tokens), (gain_ref, gain), (bias_ref, bias)))
    ]
    for load in inputs:
        load.start()
    barrier = pltpu.get_barrier_semaphore()

    with scope("greet"):
        for dx, dy in OFFSETS:
            to_y = lax.rem(y + dy, NY)
            for core, n in ((c, 1), (c, 2), (c, 0), (1 - c, 1), (1 - c, 2), (1 - c, 0)):
                if n == 0 and dx == 0 and dy == 0 and core is c:
                    continue
                pl.semaphore_signal(
                    barrier, inc=1, device_id=in_plane(dx, to_y, core, n), device_id_type=MESH
                )

    loads = [
        pltpu.make_async_copy(w, w_qkv.at[:, n * HEAD : (n + 1) * HEAD], win_sem.at[n])
        for n, w in enumerate((w_query, w_key, w_value))
    ]
    loads.append(pltpu.make_async_copy(w_inner, w_in, win_sem.at[3]))
    loads.append(pltpu.make_async_copy(w_attn, w_at, win_sem.at[4]))
    loads.append(pltpu.make_async_copy(w_outer, w_out, win_sem.at[5]))
    for load in loads:
        load.start()
    for load in inputs:
        load.wait()

    with scope("norm"):
        normed = (normalize(tokens[...].astype(F32)) * gain[...]).astype(BF16)
        for p in range(NX * NY):
            nsend[p] = normed[:, p * depth : (p + 1) * depth]
        lane = i * 2 + xh
        nrecv[0, c, lane] = nsend[i]
    with scope("barrier"):
        pl.semaphore_wait(barrier, 12 * NX * NY - 1)

    n_lane = 2 * NX * NY
    with scope("plane"):
        for n in (0, 1, 2):
            for dx, dy in OFFSETS:
                if n == 0 and dx == 0 and dy == 0:
                    continue
                target = in_plane(dx, lax.rem(y + dy, NY), c, n)
                send(nsend.at[target[0]], nrecv.at[n, c, lane], n_send, n_recv.at[n], target)

    def share_plane(n):
        wait_bytes(nrecv.at[n, 0, pl.ds(0, n_lane - (n == 0))], n_recv.at[n])
        send(nrecv.at[n, c], nrecv.at[n, c], m_send, m_recv.at[n], sibling)

    def build(n, k):
        wait_bytes(nrecv.at[n, 0], m_recv.at[n])
        for q in range(NX * NY):
            p = q % NX * NY + q // NX
            for s in range(4):
                at = q * tile + s * rows
                stage[n, at : at + rows, :] = nrecv[n, s % 2, p * 2 + s // 2].astype(F32)
        xg[k] = stage[n].astype(BF16).reshape(xg.shape[1:])

    cols = (pl.ds(0, half), pl.ds(half, half))
    piece = 8 * rows
    parts = (pl.ds(0, piece), pl.ds(piece, piece))

    def pass_on(src, dst, n, target):
        send(
            xg.at[src, c, parts[n]], xg.at[dst, c, parts[n]], r_send, r_recv.at[dst, n], target
        )

    def ring(k, n):
        if k == 0:
            for n in (0, 1, 2):
                share_plane(n)
                if n == 0:
                    build(0, 0)
            return
        if k == 4:
            for n in (0, 1):
                wait_bytes(xg.at[4, 0, parts[n]], r_recv.at[4, n])
            send(xg.at[4, c], xg.at[4, c], s_send, s_recv.at[4], sibling)
            return
        if k not in (1, 7):
            wait_bytes(xg.at[k, 0, parts[n]], r_recv.at[k, n])
        if k not in (3, 5) or (k, n) in ((5, 0), (3, 1)):
            pass_on(k, k - 1 if k > 4 else k + 1, n, z_right if k > 4 else z_left)
        if n == 1 and k not in (1, 7):
            send(xg.at[k, c], xg.at[k, c], s_send, s_recv.at[k], sibling)

    def project(g, k):
        low, high, _ = GROUPS[g]
        if k not in (0, 1, 7) and g == 0:
            wait_bytes(xg.at[k, 0], s_recv.at[k])
        w = w_qkv[...] if g == 0 else w_in[:, low - 384 : high - 384]
        pf[k, :, :, :, low:high] = jnp.dot(
            xg[k].reshape(8 * tile, depth), w, preferred_element_type=F32
        ).reshape(NY, NX, tile, high - low)

    def finish(g, k, total):
        low, high, _ = GROUPS[g]
        if g == 0:
            qkv[k] = total.astype(BF16)
            return
        low, high = low - 384, high - 384
        shift = jnp.concatenate([bias[h : h + 1] for h in range(low // HEAD, high // HEAD)], axis=1)
        inner = total + shift
        activ = 0.5 * inner * (1.0 + lax.erf(inner * math.sqrt(0.5)))
        ag[k, me, :, low:high] = activ.astype(BF16)
        if k in GATHER_AT_ONCE:
            gather_all(ag, (k,), k)
        elif k in Y_FIRST and k not in GATHER_IN_TWO:
            block = ag.at[k, me]
            send(block, block, gy_send, gr_recv.at[k], y_right)
            send(block, block, gy_send, gl_recv.at[k], y_left)
        else:
            send(ag.at[k, me], ag.at[k, me], gx_send, gx_recv.at[k], partner)

    def slices(g, k):
        width = GROUPS[g][1] - GROUPS[g][0]
        cut = (width // HEAD + k % 2) // 2 * HEAD
        return cut, pl.ds(0, cut), pl.ds(cut, width - cut)

    def start_ring(g, k, far):
        asend, arecv, _, _, _, _, a_send, ar, al, _, _, _ = groups[g][:12]
        _, right, left = slices(g, k)
        asend[k] = far.astype(BF16)
        at = (k,) + (slice(None),) * (len(asend.shape) - 2)
        send(asend.at[at + (right,)], arecv.at[at + (right,)], a_send, ar.at[k], y_right)
        send(asend.at[at + (left,)], arecv.at[at + (left,)], a_send, al.at[k], y_left)

    def relay(g, k, block):
        _, arecv, brs, brr, bls, blr, _, ar, al, b_send, br, bl = groups[g][:12]
        cut, right, left = slices(g, k)
        at = (k,) + (slice(None),) * (len(arecv.shape) - 2)
        value = block(yr)
        wait_bytes(arecv.at[at + (right,)], ar.at[k])
        brs[k] = jnp.concatenate(
            [value[..., :cut] + arecv[at + (slice(0, cut),)].astype(F32), value[..., cut:]], axis=-1
        ).astype(BF16)
        send(brs.at[k], brr.at[k], b_send, br.at[k], y_right)
        value = block(yl)
        wait_bytes(arecv.at[at + (left,)], al.at[k])
        bls[k] = jnp.concatenate(
            [value[..., :cut], value[..., cut:] + arecv[at + (slice(cut, None),)].astype(F32)], axis=-1
        ).astype(BF16)
        send(bls.at[k], blr.at[k], b_send, bl.at[k], y_left)

    def arrived(g, k, block):
        _, _, _, brr, _, blr, _, _, _, _, br, bl = groups[g][:12]
        wait_bytes(brr.at[k], br.at[k])
        wait_bytes(blr.at[k], bl.at[k])
        return block(y) + brr[k].astype(F32) + blr[k].astype(F32)

    def reduce_two(k, step):
        low, high, _ = GROUPS[1]
        dsend, drecv, d_send, d_recv = direct[1]
        sf, xsend, xrecv, x_send, x_recv = groups[1][12:]
        if step == 0:
            dsend[k] = pf[k, :, :, :, low:high].reshape(dsend.shape[1:]).astype(BF16)
            for n, to in enumerate((y2, yr, yl)):
                send(
                    dsend.at[k, pl.ds(to * NX, NX)], drecv.at[k, pl.ds(n * NX, NX)],
                    d_send, d_recv.at[k], (xl * NY + to, j),
                )
        elif step == 1:
            wait_bytes(drecv.at[k, pl.ds(0, 3 * NX)], d_recv.at[k])
            total = pf[k, y, :, :, low:high]
            for n in range(3):
                total = total + drecv[k, n * NX : (n + 1) * NX].astype(F32)
            xsend[k] = jnp.where(xl == 0, total[1], total[0]).astype(BF16)
            send(xsend.at[k], xrecv.at[k], x_send, x_recv.at[k], partner)
            sf[k] = jnp.where(xl == 0, total[0], total[1])
        elif step == 2:
            wait_bytes(xrecv.at[k], x_recv.at[k])
            finish(1, k, sf[k] + xrecv[k].astype(F32))

    def reduce_all(g, k, step):
        low, high, _ = GROUPS[g]
        dsend, drecv, d_send, d_recv = direct[g]
        if step == 0:
            dsend[k] = pf[k, :, :, :, low:high].reshape(dsend.shape[1:]).astype(BF16)
            for n, (dx, dy) in enumerate(PEERS):
                to, target = peer(dx, dy)
                send(dsend.at[k, to], drecv.at[k, n], d_send, d_recv.at[k], target)
        elif step == 1:
            wait_bytes(drecv.at[k], d_recv.at[k])
            total = pf[k, y, xl, :, low:high]
            for n in range(len(PEERS)):
                total = total + drecv[k, n].astype(F32)
            finish(g, k, total)

    def reduce(g, k, step):
        if k in REDUCE_AT_ONCE[g]:
            return reduce_all(g, k, step)
        if g == 1 and k in REDUCE_IN_TWO:
            return reduce_two(k, step)
        low, high, first = GROUPS[g]
        sf, xsend, xrecv, x_send, x_recv = groups[g][12:]
        if first == "x":
            block = lambda at: sf[k, at]
            if step == 0:
                xsend[k] = pf[k, :, 1 - xl, :, low:high].astype(BF16)
                send(xsend.at[k], xrecv.at[k], x_send, x_recv.at[k], partner)
            elif step == 1:
                wait_bytes(xrecv.at[k], x_recv.at[k])
                sf[k] = pf[k, :, xl, :, low:high] + xrecv[k].astype(F32)
                start_ring(g, k, sf[k, y2])
            elif step == 2:
                relay(g, k, block)
            else:
                finish(g, k, arrived(g, k, block))
        else:
            block = lambda at: pf[k, at, :, :, low:high]
            if step == 0:
                start_ring(g, k, block(y2))
            elif step == 1:
                relay(g, k, block)
            elif step == 2:
                total = arrived(g, k, block)
                xsend[k] = jnp.where(xl == 0, total[1], total[0]).astype(BF16)
                send(xsend.at[k], xrecv.at[k], x_send, x_recv.at[k], partner)
                sf[k] = jnp.where(xl == 0, total[0], total[1])
            else:
                wait_bytes(xrecv.at[k], x_recv.at[k])
                finish(g, k, sf[k] + xrecv[k].astype(F32))

    def spread(g, at, k):
        pair = g.at[at + (pl.ds(y * NX, NX),)]
        wait_bytes(g.at[at + (0,)], gx_recv.at[k])
        send(pair, pair, h_send, hr_recv.at[k], (xl * NY + y2, j))
        send(pair, pair, gy_send, gr_recv.at[k], y_right)
        send(pair, pair, gy_send, gl_recv.at[k], y_left)

    def spread_done(g, at, k):
        for sem in (gr_recv, gl_recv, hr_recv):
            wait_bytes(g.at[at + (pl.ds(0, NX),)], sem.at[k])

    def peer(dx, dy):
        to_x, to_y = lax.rem(xl + dx, NX), lax.rem(y + dy, NY)
        return to_y * NX + to_x, (to_x * NY + to_y, j)

    def gather_all(g, at, n):
        own = g.at[at + (me,)]
        for dx, dy in PEERS:
            send(own, own, gd_send, gd_recv.at[n], peer(dx, dy)[1])

    def gather_y(k):
        if k in GATHER_IN_TWO:
            spread(ag, (k,), k)
            return
        if k in Y_FIRST:
            wait_bytes(ag.at[k, 0], gr_recv.at[k])
            block = ag.at[k, yl * NX + xl, :, cols[0]]
            send(block, block, h_send, hr_recv.at[k], y_right)
            wait_bytes(ag.at[k, 0], gl_recv.at[k])
            block = ag.at[k, yr * NX + xl, :, cols[1]]
            send(block, block, h_send, hl_recv.at[k], y_left)
            return
        wait_bytes(ag.at[k, 0], gx_recv.at[k])
        pair = ag.at[k, pl.ds(y * NX, NX)]
        send(pair, pair, gy_send, gr_recv.at[k], y_right)
        send(pair, pair, gy_send, gl_recv.at[k], y_left)

    def gather_far(k):
        if k in GATHER_IN_TWO:
            return
        if k in Y_FIRST:
            wait_bytes(ag.at[k, 0, :, cols[0]], hr_recv.at[k])
            wait_bytes(ag.at[k, 0, :, cols[1]], hl_recv.at[k])
            for n in range(NY):
                block = ag.at[k, n * NX + xl]
                send(block, block, gx_send, gx_recv.at[k], partner)
            return
        wait_bytes(ag.at[k, pl.ds(0, NX)], gr_recv.at[k])
        block = ag.at[k, yl * NX]
        send(block, block, h_send, hr_recv.at[k], y_right)
        wait_bytes(ag.at[k, pl.ds(0, NX)], gl_recv.at[k])
        block = ag.at[k, yr * NX + 1]
        send(block, block, h_send, hl_recv.at[k], y_left)

    def gather_done(k):
        if k in GATHER_AT_ONCE:
            wait_bytes(ag.at[k, pl.ds(0, NX * NY - 1)], gd_recv.at[k])
            return
        if k in GATHER_IN_TWO:
            spread_done(ag, (k,), k)
            return
        if k in Y_FIRST:
            wait_bytes(ag.at[k, pl.ds(0, NY)], gx_recv.at[k])
            return
        wait_bytes(ag.at[k, 0], hr_recv.at[k])
        wait_bytes(ag.at[k, 0], hl_recv.at[k])

    def attend():
        query = qkv[:, :, :HEAD].reshape(8 * tile, HEAD)
        key = qkv[:, :, HEAD : 2 * HEAD].reshape(8 * tile, HEAD)
        value = qkv[:, :, 2 * HEAD :].reshape(8 * tile, HEAD)
        query_norm = normalize(query.astype(F32)).astype(BF16)
        key_norm = normalize(key.astype(F32)).astype(BF16)
        scores = lax.dot_general(
            query_norm, key_norm, (((1,), (1,)), ((), ())), preferred_element_type=F32
        )
        scores = scores * (temper[0] * (1.0 / math.sqrt(HEAD)))
        weight = jnp.exp(scores - jnp.max(scores, axis=-1, keepdims=True))
        probs = (weight / jnp.sum(weight, axis=-1, keepdims=True)).astype(BF16)
        mg[me] = jnp.dot(probs, value, preferred_element_type=F32).astype(BF16)
        if 8 in GATHER_AT_ONCE:
            gather_all(mg, (), 8)
        else:
            send(mg.at[me], mg.at[me], gx_send, gx_recv.at[8], partner)

    def project_out(k):
        gather_done(k)
        hidden = ag[k].reshape(8 * tile, depth)
        mixed = mg[:, tile * k : tile * (k + 1), :].reshape(8 * tile, HEAD)
        total = jnp.dot(hidden, w_out[...], preferred_element_type=F32)
        total = total + jnp.dot(mixed, w_at[...], preferred_element_type=F32)
        og[k] = total.reshape(og.shape[1:])
        esend[k] = og[k, 1 - c].astype(BF16)
        send(esend.at[k], erecv.at[k], e_send, e_recv.at[k], sibling)

    def combined(k):
        wait_bytes(erecv.at[k], e_recv.at[k])
        return og[k, c] + erecv[k].astype(F32)

    def reduce_out(k, n):
        span = slice(n * half, (n + 1) * half)
        if k not in summed:
            wait_bytes(erecv.at[k], e_recv.at[k])
            summed.append(k)
        value = og[k, c, :, span] + erecv[k, :, span].astype(F32)
        if k in (2, 6) or (k, n) in ((3, 0), (5, 1)):
            wait_bytes(rrecv.at[k, :, cols[n]], z_recv.at[k, n])
            value = value + rrecv[k, :, span].astype(F32)
        rsend[k, :, span] = value.astype(BF16)
        right = k < 4 or (k == 4 and n == 0)
        to = k - 1 if right else k + 1
        send(
            rsend.at[k, :, cols[n]], rrecv.at[to, :, cols[n]], z_send, z_recv.at[to, n],
            z_right if right else z_left,
        )

    def scatter_out(n, total):
        for q in range(4):
            for s in range(4):
                at = q * tile + s * rows
                fsend[n, q * 4 + s] = total[at : at + rows].astype(BF16)
        slot = i * 2 + xh
        for dx in (2, 1, 3, 0):
            to = lax.rem(x + dx, 4)
            for yy in (0, 1):
                for core in (c, 1 - c):
                    src = (yy * NX + lax.rem(to, 2)) * 4 + (to // 2) * 2 + core
                    target = in_plane(dx, 2 * c + yy, core, n)
                    if n or dx or core is not c:
                        send(fsend.at[n, src], frecv.at[n, slot], f_send, f_recv.at[n], target)
                        continue
                    own = y == 2 * c + yy

                    @pl.when(own)
                    def _():
                        frecv[n, slot] = fsend[n, src]

                    @pl.when(jnp.logical_not(own))
                    def _():
                        send(fsend.at[n, src], frecv.at[n, slot], f_send, f_recv.at[n], target)

    def finish_out(k):
        total = combined(k)
        for n in (0, 1):
            wait_bytes(rrecv.at[k, :, cols[n]], z_recv.at[k, n])
        scatter_out(2 if k == 1 else 1, total + rrecv[k].astype(F32))

    summed = []

    def step(op, n, k):
        if op == "r":
            ring(k, n)
        elif op == "b":
            build(1 if k == 1 else 2, k)
        elif op == "p":
            project(n, k)
        elif op in "qm":
            reduce("qm".index(op), k, n)
        elif op == "y":
            gather_y(k)
        elif op == "f":
            gather_far(k)
        elif op == "w":
            for load in loads[4:] if n else loads[:4]:
                load.wait()
        elif op == "a":
            attend()
        elif op == "g" and 8 in GATHER_AT_ONCE:
            if n:
                wait_bytes(mg.at[pl.ds(0, NX * NY - 1)], gd_recv.at[8])
        elif op == "g":
            (spread_done if n else spread)(mg, (), 8)
        elif op == "o":
            project_out(k)
        elif op == "s" and k in (1, 7):
            finish_out(k)
        elif op == "s":
            reduce_out(k, n)

    for word in SCHEDULE:
        name, k = word.split(".")
        with scope(f"{name}#k={k}"):
            step(name[0], int(name[1:] or 0), int(k))

    with scope("last"):
        scatter_out(0, combined(0))
    with scope("final"):
        mine = c == y // 2

        @pl.when(mine)
        def _():
            wait_bytes(frecv.at[0, pl.ds(0, n_lane - 1)], f_recv.at[0])
            wait_bytes(frecv.at[0, pl.ds(0, n_lane - 1)], f_send)

        @pl.when(jnp.logical_not(mine))
        def _():
            wait_bytes(frecv.at[0], f_recv.at[0])
            wait_bytes(frecv.at[0], f_send)

        for n in (1, 2):
            wait_bytes(frecv.at[n], f_recv.at[n])
            wait_bytes(frecv.at[n], f_send)

    for p in range(NX * NY):
        span = slice(p * depth, (p + 1) * depth)
        total = tokens[:, span].astype(F32)
        for n in range(3):
            total = total + frecv[n, 2 * p].astype(F32) + frecv[n, 2 * p + 1].astype(F32)
        out[:, span] = total.astype(BF16)

    wait_bytes(nrecv.at[0, 0, pl.ds(0, n_lane - 1)], n_send)
    wait_bytes(nrecv.at[0], n_send)
    wait_bytes(nrecv.at[:, 0], m_send)
    wait_bytes(xg.at[pl.ds(0, 5), 0], r_send)
    wait_bytes(xg.at[pl.ds(0, 5), 0], s_send)
    for g, scratch in enumerate(groups):
        once, two = len(REDUCE_AT_ONCE[g]), len(REDUCE_IN_TWO) * g
        asend, _, brs, _, bls, _, a_send, _, _, b_send, _, _, _, xsend, _, x_send, _ = scratch
        for ref, sem in ((asend, a_send), (brs, b_send), (bls, b_send)):
            wait_bytes(ref.at[pl.ds(0, NZ - once - two)], sem)
        wait_bytes(xsend.at[pl.ds(0, NZ - once)], x_send)
        if once:
            wait_bytes(direct[g][1].at[pl.ds(0, once)], direct[g][2])
        if two:
            wait_bytes(direct[g][1].at[pl.ds(0, two), pl.ds(0, 3 * NX)], direct[g][2])
    at_once = [k for k in GATHER_AT_ONCE if k < 8]
    late = len(Y_FIRST)
    n = NZ - len(at_once) - late
    for count, blocks in ((n, (1, 4, 2)), (late, (4, 2, 1))):
        for width, sem in zip(blocks, (gx_send, gy_send, h_send)):
            if count:
                wait_bytes(ag.at[pl.ds(0, count), pl.ds(0, width)], sem)
    if at_once:
        wait_bytes(ag.at[pl.ds(0, len(at_once)), pl.ds(0, NX * NY - 1)], gd_send)
    if 8 in GATHER_AT_ONCE:
        wait_bytes(mg.at[pl.ds(0, NX * NY - 1)], gd_send)
    else:
        for width, sem in zip((1, 4, 2), (gx_send, gy_send, h_send)):
            wait_bytes(mg.at[pl.ds(0, width)], sem)
    wait_bytes(esend, e_send)
    wait_bytes(rsend.at[pl.ds(0, 5)], z_send)


def group_scratch(low, high, first, tile):
    dma = pltpu.SemaphoreType.DMA
    width = high - low
    ring = (NZ, tile, width) if first == "x" else (NZ, NX, tile, width)
    swap = (NZ, NY, tile, width) if first == "x" else (NZ, tile, width)
    return tuple(pltpu.VMEM(ring, BF16) for _ in range(6)) + (
        dma, dma((8,)), dma((8,)), dma, dma((8,)), dma((8,)),
        pltpu.VMEM(swap, F32), pltpu.VMEM(swap, BF16), pltpu.VMEM(swap, BF16), dma, dma((8,)),
    )


def per_device(
    tokens, norm_gain, w_query, w_key, w_value, w_inner, bias_inner, w_attn_out, w_outer, temper
):
    rows, width = tokens.shape
    depth = w_query.shape[0]
    hidden = w_inner.shape[1]
    wide = 3 * HEAD
    tile = 4 * rows
    vmem = pl.BlockSpec(memory_space=pltpu.VMEM)
    smem = pl.BlockSpec(memory_space=pltpu.SMEM)
    hbm = pl.BlockSpec(memory_space=pl.ANY)
    dma = pltpu.SemaphoreType.DMA
    return pl.pallas_call(
        block_kernel,
        out_shape=jax.ShapeDtypeStruct((rows, width), BF16),
        in_specs=[hbm, hbm, hbm, smem] + [hbm] * 6,
        out_specs=vmem,
        scratch_shapes=[
            pltpu.VMEM((rows, width), BF16),
            pltpu.VMEM((1, width), F32),
            pltpu.VMEM((hidden // HEAD, HEAD), F32),
            pltpu.VMEM((depth, wide), BF16),
            pltpu.VMEM((depth, hidden), BF16),
            pltpu.VMEM((HEAD, depth), BF16),
            pltpu.VMEM((hidden, depth), BF16),
            pltpu.VMEM((8, rows, depth), BF16),
            pltpu.VMEM((3, 2, 16, rows, depth), BF16),
            pltpu.VMEM((3, 8 * tile, depth), F32),
            pltpu.VMEM((NZ, 2, 4 * tile, depth), BF16),
            pltpu.VMEM((NZ, NY, NX, tile, wide + hidden), F32),
            tuple(group_scratch(*g, tile) for g in GROUPS),
            tuple(
                (
                    pltpu.VMEM((NZ, NX * NY, tile, high - low), BF16),
                    pltpu.VMEM((NZ, len(PEERS), tile, high - low), BF16),
                    dma, dma((8,)),
                )
                for low, high, _ in GROUPS
            ),
            pltpu.VMEM((NZ, tile, wide), BF16),
            pltpu.VMEM((NZ, NX * NY, tile, hidden), BF16),
            pltpu.VMEM((NX * NY, 8 * tile, HEAD), BF16),
            pltpu.VMEM((NZ, 2, 4 * tile, depth), F32),
            pltpu.VMEM((NZ, 4 * tile, depth), BF16),
            pltpu.VMEM((NZ, 4 * tile, depth), BF16),
            pltpu.VMEM((NZ, 4 * tile, depth), BF16),
            pltpu.VMEM((NZ + 1, 4 * tile, depth), BF16),
            pltpu.VMEM((3, 16, rows, depth), BF16),
            pltpu.VMEM((3, 16, rows, depth), BF16),
            dma((3,)), dma((6,)), dma, dma((3,)), dma, dma((3,)), dma, dma((8, 2)), dma, dma((8,)),
            dma, dma((9,)),
            dma, dma((9,)), dma, dma((9,)), dma((9,)), dma, dma((9,)), dma((9,)),
            dma, dma((8,)), dma, dma((9, 2)), dma, dma((3,)),
        ],
        compiler_params=pltpu.CompilerParams(
            collective_id=0, has_side_effects=True, vmem_limit_bytes=60 * 1024 * 1024
        ),
        name="encoder_block",
    )(
        tokens, norm_gain.reshape(1, -1), bias_inner.reshape(-1, HEAD), temper,
        w_query, w_key, w_value, w_inner, w_attn_out, w_outer,
    )


def solution(mesh):
    return jax.shard_map(
        per_device,
        mesh=mesh,
        in_specs=(
            P(("dp", "mp"), None),
            P(),
            P("dp", "mp"),
            P("dp", "mp"),
            P("dp", "mp"),
            P("dp", "mp"),
            P("mp"),
            P("mp", "dp"),
            P("mp", "dp"),
            P("mp"),
        ),
        out_specs=P(("dp", "mp"), None),
        check_vma=False,
    )
```

```python
import functools
import math

import jax
import jax.numpy as jnp
from jax import lax
from jax.experimental import pallas as pl
from jax.experimental.pallas import tpu as pltpu
from jax.sharding import PartitionSpec as P

HEAD = 128
NX, NY, NZ = 2, 4, 8
MESH = pl.DeviceIdType.MESH
F32, BF16 = jnp.float32, jnp.bfloat16
GROUPS = ((0, 384, "x"), (384, 1152, "y"))
REDUCE_AT_ONCE = ((4, 6, 7), (4, 5))
REDUCE_IN_TWO = (0, 3)
GATHER_AT_ONCE = (4, 7)
GATHER_IN_TWO = (1,)
Y_FIRST = (5, 6)
X_THEN_ALL = ()
MIX = ((4,), (3, 5), (2, 6), (1, 7), (0,))
PLACE = {k: n for n, k in enumerate(sum(MIX, ()))}
PEERS = tuple((dx, dy) for dy in (2, 1, 3, 0) for dx in (1, 0) if dx or dy)
SCHEDULE = (
    "r.0", "w0.0", "p0.0", "q0.0", "p1.0", "m0.0", "b.7", "r0.7", "b.1", "r0.1",
    "p0.1", "q0.1", "p1.1", "r1.7", "p0.7", "r1.1", "m0.1", "q1.0", "q0.7", "p1.7",
    "m0.7", "r0.6", "r0.2", "q1.1", "m1.0", "r1.6", "q2.0", "r1.2", "m1.1", "p0.6",
    "p1.6", "m0.6", "q0.6", "m1.7", "q2.1", "p0.2", "q0.2", "r0.5", "p1.2", "m0.2",
    "r1.5", "r0.3", "q3.0", "r1.3", "m1.6", "p0.3", "q0.3", "p1.3", "p0.5", "m0.3",
    "q1.7", "q0.5", "q1.2", "p1.5", "m0.5", "r.4", "q1.3", "p0.4", "m2.6", "p1.4",
    "m2.1", "m0.4", "m1.3", "m1.2", "q1.5", "q0.4", "m2.0", "q2.3", "q1.6", "m3.6",
    "q2.2", "m1.5", "q3.1", "m2.3", "m2.2", "q2.5", "m1.4", "q1.4", "y.3", "y.5",
    "q3.3", "y.6", "m3.1", "q3.5", "q3.2", "m3.2", "a.0", "f.3", "y.2", "y.0",
    "f.5", "y.1", "m2.7", "w1.0", "o.4", "f.6", "s1.4", "s0.4", "o.3", "f.2",
    "o.5", "m3.7", "s1.3", "s0.5", "s1.5", "s0.3", "o.6", "o.2", "f.0", "s1.2",
    "s0.6", "s0.2", "s1.6", "o.1", "o.7", "o.0", "s0.1", "s0.7",
)
OFFSETS = sorted(
    ((dx, dy) for dx in range(4) for dy in range(NY)),
    key=lambda o: -(min(o[0], 4 - o[0]) + min(o[1], NY - o[1])),
)

scope = jax.named_scope


def normalize(values):
    center = values - jnp.mean(values, axis=-1, keepdims=True)
    spread = jnp.mean(center * center, axis=-1, keepdims=True)
    return center * lax.rsqrt(spread + 1e-06)


def wait_bytes(ref, sem):
    pltpu.make_async_copy(ref, ref, sem).wait()


def send(src, dst, send_sem, recv_sem, target):
    pltpu.make_async_remote_copy(
        src_ref=src, dst_ref=dst, send_sem=send_sem, recv_sem=recv_sem,
        device_id=target, device_id_type=MESH,
    ).start()


def block_kernel(
    tokens_ref, gain_ref, bias_ref, temper, w_query, w_key, w_value, w_inner, w_attn, w_outer,
    out,
    tokens, gain, bias, w_qkv, w_in, w_at, w_out, nsend, nrecv, stage, xg, pf, groups,
    direct, qkv, ag, mg, og, esend, erecv, rsend, rrecv, fsend, frecv,
    in_sem, win_sem, n_send, n_recv, m_send, m_recv, r_send, r_recv, s_send, s_recv,
    gd_send, gd_recv, gx_send, gx_recv, gy_send, gr_recv, gl_recv, h_send, hr_recv, hl_recv,
    e_send, e_recv, z_send, z_recv, f_send, f_recv,
):
    rows, depth = nsend.shape[1:]
    tile = 4 * rows
    half = depth // 2
    i, j = lax.axis_index("dp"), lax.axis_index("mp")
    xl, y = i // NY, lax.rem(i, NY)
    z, xh, c = j // 4, lax.rem(j // 2, 2), lax.rem(j, 2)
    x, me = xh * 2 + xl, y * NX + xl
    yr, yl, y2 = lax.rem(y + 1, NY), lax.rem(y + NY - 1, NY), lax.rem(y + 2, NY)
    zr, zl = lax.rem(z + 1, NZ), lax.rem(z + NZ - 1, NZ)
    sibling = (i, z * 4 + xh * 2 + 1 - c)
    partner = ((1 - xl) * NY + y, j)
    y_right, y_left = (xl * NY + yr, j), (xl * NY + yl, j)
    z_right, z_left = (i, zr * 4 + xh * 2 + c), (i, zl * 4 + xh * 2 + c)

    planes = (z, zl, zr)

    def in_plane(dx, to_y, core, n=0):
        to = lax.rem(x + dx, 4)
        return (lax.rem(to, 2) * NY + to_y, planes[n] * 4 + (to // 2) * 2 + core)

    inputs = [
        pltpu.make_async_copy(src, dst, in_sem.at[n])
        for n, (src, dst) in enumerate(((tokens_ref, tokens), (gain_ref, gain), (bias_ref, bias)))
    ]
    for load in inputs:
        load.start()
    barrier = pltpu.get_barrier_semaphore()

    with scope("greet"):
        for dx, dy in OFFSETS:
            to_y = lax.rem(y + dy, NY)
            for core, n in ((c, 1), (c, 2), (c, 0), (1 - c, 1), (1 - c, 2), (1 - c, 0)):
                if n == 0 and dx == 0 and dy == 0 and core is c:
                    continue
                pl.semaphore_signal(
                    barrier, inc=1, device_id=in_plane(dx, to_y, core, n), device_id_type=MESH
                )

    loads = [
        pltpu.make_async_copy(w, w_qkv.at[:, n * HEAD : (n + 1) * HEAD], win_sem.at[n])
        for n, w in enumerate((w_query, w_key, w_value))
    ]
    loads.append(pltpu.make_async_copy(w_inner, w_in, win_sem.at[3]))
    loads.append(pltpu.make_async_copy(w_attn, w_at, win_sem.at[4]))
    loads.append(pltpu.make_async_copy(w_outer, w_out, win_sem.at[5]))
    for load in loads:
        load.start()
    for load in inputs:
        load.wait()

    with scope("norm"):
        normed = (normalize(tokens[...].astype(F32)) * gain[...]).astype(BF16)
        for p in range(NX * NY):
            nsend[p] = normed[:, p * depth : (p + 1) * depth]
        lane = i * 2 + xh
        nrecv[0, c, lane] = nsend[i]
    with scope("barrier"):
        pl.semaphore_wait(barrier, 12 * NX * NY - 1)

    n_lane = 2 * NX * NY
    with scope("plane"):
        for n in (0, 1, 2):
            for dx, dy in OFFSETS:
                if n == 0 and dx == 0 and dy == 0:
                    continue
                target = in_plane(dx, lax.rem(y + dy, NY), c, n)
                send(nsend.at[target[0]], nrecv.at[n, c, lane], n_send, n_recv.at[n], target)

    def share_plane(n):
        wait_bytes(nrecv.at[n, 0, pl.ds(0, n_lane - (n == 0))], n_recv.at[n])
        send(nrecv.at[n, c], nrecv.at[n, c], m_send, m_recv.at[n], sibling)

    def build(n, k):
        wait_bytes(nrecv.at[n, 0], m_recv.at[n])
        for q in range(NX * NY):
            p = q % NX * NY + q // NX
            for s in range(4):
                at = q * tile + s * rows
                stage[n, at : at + rows, :] = nrecv[n, s % 2, p * 2 + s // 2].astype(F32)
        xg[k] = stage[n].astype(BF16).reshape(xg.shape[1:])

    cols = (pl.ds(0, half), pl.ds(half, half))
    piece = 8 * rows
    parts = (pl.ds(0, piece), pl.ds(piece, piece))

    def pass_on(src, dst, n, target):
        send(
            xg.at[src, c, parts[n]], xg.at[dst, c, parts[n]], r_send, r_recv.at[dst, n], target
        )

    def ring(k, n):
        if k == 0:
            for n in (0, 1, 2):
                share_plane(n)
                if n == 0:
                    build(0, 0)
            return
        if k == 4:
            for n in (0, 1):
                wait_bytes(xg.at[4, 0, parts[n]], r_recv.at[4, n])
            send(xg.at[4, c], xg.at[4, c], s_send, s_recv.at[4], sibling)
            return
        if k not in (1, 7):
            wait_bytes(xg.at[k, 0, parts[n]], r_recv.at[k, n])
        if k not in (3, 5) or (k, n) in ((5, 0), (3, 1)):
            pass_on(k, k - 1 if k > 4 else k + 1, n, z_right if k > 4 else z_left)
        if n == 1 and k not in (1, 7):
            send(xg.at[k, c], xg.at[k, c], s_send, s_recv.at[k], sibling)

    def project(g, k):
        low, high, _ = GROUPS[g]
        if k not in (0, 1, 7) and g == 0:
            wait_bytes(xg.at[k, 0], s_recv.at[k])
        w = w_qkv[...] if g == 0 else w_in[:, low - 384 : high - 384]
        pf[k, :, :, :, low:high] = jnp.dot(
            xg[k].reshape(8 * tile, depth), w, preferred_element_type=F32
        ).reshape(NY, NX, tile, high - low)

    def finish(g, k, total):
        low, high, _ = GROUPS[g]
        if g == 0:
            qkv[PLACE[k]] = total.astype(BF16)
            return
        low, high = low - 384, high - 384
        shift = jnp.concatenate([bias[h : h + 1] for h in range(low // HEAD, high // HEAD)], axis=1)
        inner = total + shift
        activ = 0.5 * inner * (1.0 + lax.erf(inner * math.sqrt(0.5)))
        ag[k, me, :, low:high] = activ.astype(BF16)
        if k in GATHER_AT_ONCE:
            gather_all(ag, (k,), k)
        elif k in Y_FIRST and k not in GATHER_IN_TWO:
            block = ag.at[k, me]
            send(block, block, gy_send, gr_recv.at[k], y_right)
            send(block, block, gy_send, gl_recv.at[k], y_left)
        else:
            send(ag.at[k, me], ag.at[k, me], gx_send, gx_recv.at[k], partner)

    def slices(g, k):
        width = GROUPS[g][1] - GROUPS[g][0]
        cut = (width // HEAD + k % 2) // 2 * HEAD
        return cut, pl.ds(0, cut), pl.ds(cut, width - cut)

    def start_ring(g, k, far):
        asend, arecv, _, _, _, _, a_send, ar, al, _, _, _ = groups[g][:12]
        _, right, left = slices(g, k)
        asend[k] = far.astype(BF16)
        at = (k,) + (slice(None),) * (len(asend.shape) - 2)
        send(asend.at[at + (right,)], arecv.at[at + (right,)], a_send, ar.at[k], y_right)
        send(asend.at[at + (left,)], arecv.at[at + (left,)], a_send, al.at[k], y_left)

    def relay(g, k, block):
        _, arecv, brs, brr, bls, blr, _, ar, al, b_send, br, bl = groups[g][:12]
        cut, right, left = slices(g, k)
        at = (k,) + (slice(None),) * (len(arecv.shape) - 2)
        value = block(yr)
        wait_bytes(arecv.at[at + (right,)], ar.at[k])
        brs[k] = jnp.concatenate(
            [value[..., :cut] + arecv[at + (slice(0, cut),)].astype(F32), value[..., cut:]], axis=-1
        ).astype(BF16)
        send(brs.at[k], brr.at[k], b_send, br.at[k], y_right)
        value = block(yl)
        wait_bytes(arecv.at[at + (left,)], al.at[k])
        bls[k] = jnp.concatenate(
            [value[..., :cut], value[..., cut:] + arecv[at + (slice(cut, None),)].astype(F32)], axis=-1
        ).astype(BF16)
        send(bls.at[k], blr.at[k], b_send, bl.at[k], y_left)

    def arrived(g, k, block):
        _, _, _, brr, _, blr, _, _, _, _, br, bl = groups[g][:12]
        wait_bytes(brr.at[k], br.at[k])
        wait_bytes(blr.at[k], bl.at[k])
        return block(y) + brr[k].astype(F32) + blr[k].astype(F32)

    def reduce_two(k, step):
        low, high, _ = GROUPS[1]
        dsend, drecv, d_send, d_recv = direct[1]
        sf, xsend, xrecv, x_send, x_recv = groups[1][12:]
        if step == 0:
            dsend[k] = pf[k, :, :, :, low:high].reshape(dsend.shape[1:]).astype(BF16)
            for n, to in enumerate((y2, yr, yl)):
                send(
                    dsend.at[k, pl.ds(to * NX, NX)], drecv.at[k, pl.ds(n * NX, NX)],
                    d_send, d_recv.at[k], (xl * NY + to, j),
                )
        elif step == 1:
            wait_bytes(drecv.at[k, pl.ds(0, 3 * NX)], d_recv.at[k])
            total = pf[k, y, :, :, low:high]
            for n in range(3):
                total = total + drecv[k, n * NX : (n + 1) * NX].astype(F32)
            xsend[k] = jnp.where(xl == 0, total[1], total[0]).astype(BF16)
            send(xsend.at[k], xrecv.at[k], x_send, x_recv.at[k], partner)
            sf[k] = jnp.where(xl == 0, total[0], total[1])
        elif step == 2:
            wait_bytes(xrecv.at[k], x_recv.at[k])
            finish(1, k, sf[k] + xrecv[k].astype(F32))

    def reduce_x_then_all(k, step):
        low, high, _ = GROUPS[0]
        dsend, drecv, d_send, d_recv = direct[0]
        sf, xsend, xrecv, x_send, x_recv = groups[0][12:]
        if step == 0:
            xsend[k] = pf[k, :, 1 - xl, :, low:high].astype(BF16)
            send(xsend.at[k], xrecv.at[k], x_send, x_recv.at[k], partner)
        elif step == 1:
            wait_bytes(xrecv.at[k], x_recv.at[k])
            sf[k] = pf[k, :, xl, :, low:high] + xrecv[k].astype(F32)
            dsend[k, :NY] = sf[k].astype(BF16)
            for n, to in enumerate((y2, yr, yl)):
                send(dsend.at[k, to], drecv.at[k, n], d_send, d_recv.at[k], (xl * NY + to, j))
        elif step == 2:
            wait_bytes(drecv.at[k, pl.ds(0, 3)], d_recv.at[k])
            total = sf[k, y]
            for n in range(3):
                total = total + drecv[k, n].astype(F32)
            finish(0, k, total)

    def reduce_all(g, k, step):
        low, high, _ = GROUPS[g]
        dsend, drecv, d_send, d_recv = direct[g]
        if step == 0:
            dsend[k] = pf[k, :, :, :, low:high].reshape(dsend.shape[1:]).astype(BF16)
            for n, (dx, dy) in enumerate(PEERS):
                to, target = peer(dx, dy)
                send(dsend.at[k, to], drecv.at[k, n], d_send, d_recv.at[k], target)
        elif step == 1:
            wait_bytes(drecv.at[k], d_recv.at[k])
            total = pf[k, y, xl, :, low:high]
            for n in range(len(PEERS)):
                total = total + drecv[k, n].astype(F32)
            finish(g, k, total)

    def reduce(g, k, step):
        if k in REDUCE_AT_ONCE[g]:
            return reduce_all(g, k, step)
        if g == 0 and k in X_THEN_ALL:
            return reduce_x_then_all(k, step)
        if g == 1 and k in REDUCE_IN_TWO:
            return reduce_two(k, step)
        low, high, first = GROUPS[g]
        sf, xsend, xrecv, x_send, x_recv = groups[g][12:]
        if first == "x":
            block = lambda at: sf[k, at]
            if step == 0:
                xsend[k] = pf[k, :, 1 - xl, :, low:high].astype(BF16)
                send(xsend.at[k], xrecv.at[k], x_send, x_recv.at[k], partner)
            elif step == 1:
                wait_bytes(xrecv.at[k], x_recv.at[k])
                sf[k] = pf[k, :, xl, :, low:high] + xrecv[k].astype(F32)
                start_ring(g, k, sf[k, y2])
            elif step == 2:
                relay(g, k, block)
            else:
                finish(g, k, arrived(g, k, block))
        else:
            block = lambda at: pf[k, at, :, :, low:high]
            if step == 0:
                start_ring(g, k, block(y2))
            elif step == 1:
                relay(g, k, block)
            elif step == 2:
                total = arrived(g, k, block)
                xsend[k] = jnp.where(xl == 0, total[1], total[0]).astype(BF16)
                send(xsend.at[k], xrecv.at[k], x_send, x_recv.at[k], partner)
                sf[k] = jnp.where(xl == 0, total[0], total[1])
            else:
                wait_bytes(xrecv.at[k], x_recv.at[k])
                finish(g, k, sf[k] + xrecv[k].astype(F32))

    def spread(g, at, k):
        pair = g.at[at + (pl.ds(y * NX, NX),)]
        wait_bytes(g.at[at + (0,)], gx_recv.at[k])
        send(pair, pair, h_send, hr_recv.at[k], (xl * NY + y2, j))
        send(pair, pair, gy_send, gr_recv.at[k], y_right)
        send(pair, pair, gy_send, gl_recv.at[k], y_left)

    def spread_done(g, at, k):
        for sem in (gr_recv, gl_recv, hr_recv):
            wait_bytes(g.at[at + (pl.ds(0, NX),)], sem.at[k])

    def peer(dx, dy):
        to_x, to_y = lax.rem(xl + dx, NX), lax.rem(y + dy, NY)
        return to_y * NX + to_x, (to_x * NY + to_y, j)

    def gather_all(g, at, n):
        own = g.at[at + (me,)]
        for dx, dy in PEERS:
            send(own, own, gd_send, gd_recv.at[n], peer(dx, dy)[1])

    def gather_y(k):
        if k in GATHER_IN_TWO:
            spread(ag, (k,), k)
            return
        if k in Y_FIRST:
            wait_bytes(ag.at[k, 0], gr_recv.at[k])
            block = ag.at[k, yl * NX + xl, :, cols[0]]
            send(block, block, h_send, hr_recv.at[k], y_right)
            wait_bytes(ag.at[k, 0], gl_recv.at[k])
            block = ag.at[k, yr * NX + xl, :, cols[1]]
            send(block, block, h_send, hl_recv.at[k], y_left)
            return
        wait_bytes(ag.at[k, 0], gx_recv.at[k])
        pair = ag.at[k, pl.ds(y * NX, NX)]
        send(pair, pair, gy_send, gr_recv.at[k], y_right)
        send(pair, pair, gy_send, gl_recv.at[k], y_left)

    def gather_far(k):
        if k in GATHER_IN_TWO:
            return
        if k in Y_FIRST:
            wait_bytes(ag.at[k, 0, :, cols[0]], hr_recv.at[k])
            wait_bytes(ag.at[k, 0, :, cols[1]], hl_recv.at[k])
            for n in range(NY):
                block = ag.at[k, n * NX + xl]
                send(block, block, gx_send, gx_recv.at[k], partner)
            return
        wait_bytes(ag.at[k, pl.ds(0, NX)], gr_recv.at[k])
        block = ag.at[k, yl * NX]
        send(block, block, h_send, hr_recv.at[k], y_right)
        wait_bytes(ag.at[k, pl.ds(0, NX)], gl_recv.at[k])
        block = ag.at[k, yr * NX + 1]
        send(block, block, h_send, hl_recv.at[k], y_left)

    def gather_done(k):
        if k in GATHER_AT_ONCE:
            wait_bytes(ag.at[k, pl.ds(0, NX * NY - 1)], gd_recv.at[k])
            return
        if k in GATHER_IN_TWO:
            spread_done(ag, (k,), k)
            return
        if k in Y_FIRST:
            wait_bytes(ag.at[k, pl.ds(0, NY)], gx_recv.at[k])
            return
        wait_bytes(ag.at[k, 0], hr_recv.at[k])
        wait_bytes(ag.at[k, 0], hl_recv.at[k])

    def attend():
        query = qkv[:, :, :HEAD].reshape(8 * tile, HEAD)
        key = qkv[:, :, HEAD : 2 * HEAD].reshape(8 * tile, HEAD)
        value = qkv[:, :, 2 * HEAD :].reshape(8 * tile, HEAD)
        query_norm = normalize(query.astype(F32)).astype(BF16)
        key_norm = normalize(key.astype(F32)).astype(BF16)
        scores = lax.dot_general(
            query_norm, key_norm, (((1,), (1,)), ((), ())), preferred_element_type=F32
        )
        scores = scores * (temper[0] * (1.0 / math.sqrt(HEAD)))
        weight = jnp.exp(scores - jnp.max(scores, axis=-1, keepdims=True))
        probs = (weight / jnp.sum(weight, axis=-1, keepdims=True)).astype(BF16)
        mg[me] = jnp.dot(probs, value, preferred_element_type=F32).astype(BF16)
        for n, group in enumerate(MIX):
            own = mg.at[me, pl.ds(PLACE[group[0]] * tile, len(group) * tile)]
            for dx, dy in PEERS:
                send(own, own, gd_send, gd_recv.at[8 + n], peer(dx, dy)[1])

    mixed_here = []

    def mixed_done(k):
        for n, group in enumerate(MIX):
            if k in group and n not in mixed_here:
                wait_bytes(mg.at[pl.ds(0, len(PEERS)), pl.ds(0, len(group) * tile)], gd_recv.at[8 + n])
                mixed_here.append(n)

    def project_out(k):
        gather_done(k)
        mixed_done(k)
        hidden = ag[k].reshape(8 * tile, depth)
        at = tile * PLACE[k]
        mixed = mg[:, at : at + tile, :].reshape(8 * tile, HEAD)
        total = jnp.dot(hidden, w_out[...], preferred_element_type=F32)
        total = total + jnp.dot(mixed, w_at[...], preferred_element_type=F32)
        og[k] = total.reshape(og.shape[1:])
        esend[k] = og[k, 1 - c].astype(BF16)
        send(esend.at[k], erecv.at[k], e_send, e_recv.at[k], sibling)

    def combined(k):
        wait_bytes(erecv.at[k], e_recv.at[k])
        return og[k, c] + erecv[k].astype(F32)

    def reduce_out(k, n):
        span = slice(n * half, (n + 1) * half)
        if k not in summed:
            wait_bytes(erecv.at[k], e_recv.at[k])
            summed.append(k)
        value = og[k, c, :, span] + erecv[k, :, span].astype(F32)
        if k in (2, 6) or (k, n) in ((3, 0), (5, 1)):
            wait_bytes(rrecv.at[k, :, cols[n]], z_recv.at[k, n])
            value = value + rrecv[k, :, span].astype(F32)
        rsend[k, :, span] = value.astype(BF16)
        right = k < 4 or (k == 4 and n == 0)
        to = k - 1 if right else k + 1
        send(
            rsend.at[k, :, cols[n]], rrecv.at[to, :, cols[n]], z_send, z_recv.at[to, n],
            z_right if right else z_left,
        )

    def scatter_out(n, total):
        for q in range(4):
            for s in range(4):
                at = q * tile + s * rows
                fsend[n, q * 4 + s] = total[at : at + rows].astype(BF16)
        slot = i * 2 + xh
        for dx in (2, 1, 3, 0):
            to = lax.rem(x + dx, 4)
            for yy in (0, 1):
                for core in (c, 1 - c):
                    src = (yy * NX + lax.rem(to, 2)) * 4 + (to // 2) * 2 + core
                    target = in_plane(dx, 2 * c + yy, core, n)
                    if n or dx or core is not c:
                        send(fsend.at[n, src], frecv.at[n, slot], f_send, f_recv.at[n], target)
                        continue
                    own = y == 2 * c + yy

                    @pl.when(own)
                    def _():
                        frecv[n, slot] = fsend[n, src]

                    @pl.when(jnp.logical_not(own))
                    def _():
                        send(fsend.at[n, src], frecv.at[n, slot], f_send, f_recv.at[n], target)

    def finish_out(k):
        total = combined(k)
        for n in (0, 1):
            wait_bytes(rrecv.at[k, :, cols[n]], z_recv.at[k, n])
        scatter_out(2 if k == 1 else 1, total + rrecv[k].astype(F32))

    summed = []

    def step(op, n, k):
        if op == "r":
            ring(k, n)
        elif op == "b":
            build(1 if k == 1 else 2, k)
        elif op == "p":
            project(n, k)
        elif op in "qm":
            reduce("qm".index(op), k, n)
        elif op == "y":
            gather_y(k)
        elif op == "f":
            gather_far(k)
        elif op == "w":
            for load in loads[4:] if n else loads[:4]:
                load.wait()
        elif op == "a":
            attend()
        elif op == "o":
            project_out(k)
        elif op == "s" and k in (1, 7):
            finish_out(k)
        elif op == "s":
            reduce_out(k, n)

    for word in SCHEDULE:
        name, k = word.split(".")
        with scope(f"{name}#k={k}"):
            step(name[0], int(name[1:] or 0), int(k))

    with scope("last"):
        scatter_out(0, combined(0))
    with scope("final"):
        mine = c == y // 2

        @pl.when(mine)
        def _():
            wait_bytes(frecv.at[0, pl.ds(0, n_lane - 1)], f_recv.at[0])
            wait_bytes(frecv.at[0, pl.ds(0, n_lane - 1)], f_send)

        @pl.when(jnp.logical_not(mine))
        def _():
            wait_bytes(frecv.at[0], f_recv.at[0])
            wait_bytes(frecv.at[0], f_send)

        for n in (1, 2):
            wait_bytes(frecv.at[n], f_recv.at[n])
            wait_bytes(frecv.at[n], f_send)

    for p in range(NX * NY):
        span = slice(p * depth, (p + 1) * depth)
        total = tokens[:, span].astype(F32)
        for n in range(3):
            total = total + frecv[n, 2 * p].astype(F32) + frecv[n, 2 * p + 1].astype(F32)
        out[:, span] = total.astype(BF16)

    wait_bytes(nrecv.at[0, 0, pl.ds(0, n_lane - 1)], n_send)
    wait_bytes(nrecv.at[0], n_send)
    wait_bytes(nrecv.at[:, 0], m_send)
    wait_bytes(xg.at[pl.ds(0, 5), 0], r_send)
    wait_bytes(xg.at[pl.ds(0, 5), 0], s_send)
    for g, scratch in enumerate(groups):
        once, two = len(REDUCE_AT_ONCE[g]), len((X_THEN_ALL, REDUCE_IN_TWO)[g])
        asend, _, brs, _, bls, _, a_send, _, _, b_send, _, _, _, xsend, _, x_send, _ = scratch
        for ref, sem in ((asend, a_send), (brs, b_send), (bls, b_send)):
            wait_bytes(ref.at[pl.ds(0, NZ - once - two)], sem)
        wait_bytes(xsend.at[pl.ds(0, NZ - once)], x_send)
        if once:
            wait_bytes(direct[g][1].at[pl.ds(0, once)], direct[g][2])
        if two:
            wait_bytes(direct[g][1].at[pl.ds(0, two), pl.ds(0, 3 + 3 * g)], direct[g][2])
    at_once = [k for k in GATHER_AT_ONCE if k < 8]
    late = len(Y_FIRST)
    n = NZ - len(at_once) - late
    for count, blocks in ((n, (1, 4, 2)), (late, (4, 2, 1))):
        for width, sem in zip(blocks, (gx_send, gy_send, h_send)):
            if count:
                wait_bytes(ag.at[pl.ds(0, count), pl.ds(0, width)], sem)
    if at_once:
        wait_bytes(ag.at[pl.ds(0, len(at_once)), pl.ds(0, NX * NY - 1)], gd_send)
    wait_bytes(mg.at[pl.ds(0, NX * NY - 1)], gd_send)
    wait_bytes(esend, e_send)
    wait_bytes(rsend.at[pl.ds(0, 5)], z_send)


def group_scratch(low, high, first, tile):
    dma = pltpu.SemaphoreType.DMA
    width = high - low
    ring = (NZ, tile, width) if first == "x" else (NZ, NX, tile, width)
    swap = (NZ, NY, tile, width) if first == "x" else (NZ, tile, width)
    return tuple(pltpu.VMEM(ring, BF16) for _ in range(6)) + (
        dma, dma((8,)), dma((8,)), dma, dma((8,)), dma((8,)),
        pltpu.VMEM(swap, F32), pltpu.VMEM(swap, BF16), pltpu.VMEM(swap, BF16), dma, dma((8,)),
    )


def per_device(
    tokens, norm_gain, w_query, w_key, w_value, w_inner, bias_inner, w_attn_out, w_outer, temper
):
    rows, width = tokens.shape
    depth = w_query.shape[0]
    hidden = w_inner.shape[1]
    wide = 3 * HEAD
    tile = 4 * rows
    vmem = pl.BlockSpec(memory_space=pltpu.VMEM)
    smem = pl.BlockSpec(memory_space=pltpu.SMEM)
    hbm = pl.BlockSpec(memory_space=pl.ANY)
    dma = pltpu.SemaphoreType.DMA
    return pl.pallas_call(
        block_kernel,
        out_shape=jax.ShapeDtypeStruct((rows, width), BF16),
        in_specs=[hbm, hbm, hbm, smem] + [hbm] * 6,
        out_specs=vmem,
        scratch_shapes=[
            pltpu.VMEM((rows, width), BF16),
            pltpu.VMEM((1, width), F32),
            pltpu.VMEM((hidden // HEAD, HEAD), F32),
            pltpu.VMEM((depth, wide), BF16),
            pltpu.VMEM((depth, hidden), BF16),
            pltpu.VMEM((HEAD, depth), BF16),
            pltpu.VMEM((hidden, depth), BF16),
            pltpu.VMEM((8, rows, depth), BF16),
            pltpu.VMEM((3, 2, 16, rows, depth), BF16),
            pltpu.VMEM((3, 8 * tile, depth), F32),
            pltpu.VMEM((NZ, 2, 4 * tile, depth), BF16),
            pltpu.VMEM((NZ, NY, NX, tile, wide + hidden), F32),
            tuple(group_scratch(*g, tile) for g in GROUPS),
            tuple(
                (
                    pltpu.VMEM((NZ, NX * NY, tile, high - low), BF16),
                    pltpu.VMEM((NZ, len(PEERS), tile, high - low), BF16),
                    dma, dma((8,)),
                )
                for low, high, _ in GROUPS
            ),
            pltpu.VMEM((NZ, tile, wide), BF16),
            pltpu.VMEM((NZ, NX * NY, tile, hidden), BF16),
            pltpu.VMEM((NX * NY, 8 * tile, HEAD), BF16),
            pltpu.VMEM((NZ, 2, 4 * tile, depth), F32),
            pltpu.VMEM((NZ, 4 * tile, depth), BF16),
            pltpu.VMEM((NZ, 4 * tile, depth), BF16),
            pltpu.VMEM((NZ, 4 * tile, depth), BF16),
            pltpu.VMEM((NZ + 1, 4 * tile, depth), BF16),
            pltpu.VMEM((3, 16, rows, depth), BF16),
            pltpu.VMEM((3, 16, rows, depth), BF16),
            dma((3,)), dma((6,)), dma, dma((3,)), dma, dma((3,)), dma, dma((8, 2)), dma, dma((8,)),
            dma, dma((13,)),
            dma, dma((9,)), dma, dma((9,)), dma((9,)), dma, dma((9,)), dma((9,)),
            dma, dma((8,)), dma, dma((9, 2)), dma, dma((3,)),
        ],
        compiler_params=pltpu.CompilerParams(
            collective_id=0, has_side_effects=True, vmem_limit_bytes=60 * 1024 * 1024
        ),
        name="encoder_block",
    )(
        tokens, norm_gain.reshape(1, -1), bias_inner.reshape(-1, HEAD), temper,
        w_query, w_key, w_value, w_inner, w_attn_out, w_outer,
    )


def solution(mesh):
    return jax.shard_map(
        per_device,
        mesh=mesh,
        in_specs=(
            P(("dp", "mp"), None),
            P(),
            P("dp", "mp"),
            P("dp", "mp"),
            P("dp", "mp"),
            P("dp", "mp"),
            P("mp"),
            P("mp", "dp"),
            P("mp", "dp"),
            P("mp"),
        ),
        out_specs=P(("dp", "mp"), None),
        check_vma=False,
    )
```

```python
import functools
import math

import jax
import jax.numpy as jnp
from jax import lax
from jax.experimental import pallas as pl
from jax.experimental.pallas import tpu as pltpu
from jax.sharding import PartitionSpec as P

HEAD = 128
NX, NY, NZ = 2, 4, 8
MESH = pl.DeviceIdType.MESH
F32, BF16 = jnp.float32, jnp.bfloat16
GROUPS = ((0, 384, "x"), (384, 1152, "y"))
REDUCE_AT_ONCE = ((1,), (4, 5))
REDUCE_IN_TWO = ()
GATHER_AT_ONCE = (4,)
GATHER_IN_TWO = (1, 2, 3)
Y_FIRST = (5, 6, 7)
X_THEN_ALL = (2,)
MIX = ((4,), (3, 5), (2, 6), (1, 7), (0,))
PLACE = {k: n for n, k in enumerate(sum(MIX, ()))}
PEERS = tuple((dx, dy) for dy in (2, 1, 3, 0) for dx in (1, 0) if dx or dy)
SCHEDULE = (
    "r.0", "w0.0", "p0.0", "p1.0", "q0.0", "b.1", "r0.1", "r1.1", "m0.0", "b.7",
    "p0.7", "r0.7", "p0.1", "p1.1", "p1.7", "m0.7", "r1.7", "q0.1", "m0.1", "q0.7",
    "m1.0", "r0.2", "q1.0", "r0.6", "r1.2", "m1.7", "r1.6", "p0.2", "p1.2", "m0.2",
    "p0.6", "q0.6", "m1.1", "q1.7", "m2.0", "p1.6", "q0.2", "q2.0", "r0.5", "r0.3",
    "q1.1", "r1.3", "r1.5", "m0.6", "p0.3", "m1.2", "q0.3", "p0.5", "p1.5", "q1.6",
    "m0.5", "q3.0", "r.4", "q0.5", "p1.3", "m0.3", "p0.4", "q1.3", "m2.7", "m1.6",
    "q0.4", "p1.4", "m0.4", "m1.3", "q1.5", "m2.2", "q1.2", "q1.4", "m3.0", "q2.7",
    "m2.1", "m2.6", "m3.7", "m1.5", "q2.3", "q2.6", "m2.3", "q2.5", "q2.4", "m1.4",
    "q2.2", "m3.3", "q3.7", "q3.6", "y.5", "q3.3", "y.7", "m3.2", "q3.5", "m3.6",
    "q3.4", "a.0", "f.5", "y.6", "m3.1", "y.3", "y.0", "w1.0", "o.4", "f.6",
    "y.2", "s1.4", "s0.4", "o.5", "o.3", "f.0", "s0.5", "s0.3", "s1.5", "y.1",
    "s1.3", "o.6", "f.7", "o.2", "s0.6", "o.0", "s0.2", "s1.6", "s1.2", "o.1",
    "o.7", "s0.7", "s0.1",
)
OFFSETS = sorted(
    ((dx, dy) for dx in range(4) for dy in range(NY)),
    key=lambda o: -(min(o[0], 4 - o[0]) + min(o[1], NY - o[1])),
)

scope = jax.named_scope


def normalize(values):
    center = values - jnp.mean(values, axis=-1, keepdims=True)
    spread = jnp.mean(center * center, axis=-1, keepdims=True)
    return center * lax.rsqrt(spread + 1e-06)


def wait_bytes(ref, sem):
    pltpu.make_async_copy(ref, ref, sem).wait()


def send(src, dst, send_sem, recv_sem, target):
    pltpu.make_async_remote_copy(
        src_ref=src, dst_ref=dst, send_sem=send_sem, recv_sem=recv_sem,
        device_id=target, device_id_type=MESH,
    ).start()


def block_kernel(
    tokens_ref, gain_ref, bias_ref, temper, w_query, w_key, w_value, w_inner, w_attn, w_outer,
    out,
    tokens, gain, bias, w_qkv, w_in, w_at, w_out, nsend, nrecv, stage, xg, pf, groups,
    direct, qkv, ag, mg, og, esend, erecv, rsend, rrecv, fsend, frecv,
    in_sem, win_sem, n_send, n_recv, m_send, m_recv, r_send, r_recv, s_send, s_recv,
    gd_send, gd_recv, gx_send, gx_recv, gy_send, gr_recv, gl_recv, h_send, hr_recv, hl_recv,
    e_send, e_recv, z_send, z_recv, f_send, f_recv,
):
    rows, depth = nsend.shape[1:]
    tile = 4 * rows
    half = depth // 2
    i, j = lax.axis_index("dp"), lax.axis_index("mp")
    xl, y = i // NY, lax.rem(i, NY)
    z, xh, c = j // 4, lax.rem(j // 2, 2), lax.rem(j, 2)
    x, me = xh * 2 + xl, y * NX + xl
    yr, yl, y2 = lax.rem(y + 1, NY), lax.rem(y + NY - 1, NY), lax.rem(y + 2, NY)
    zr, zl = lax.rem(z + 1, NZ), lax.rem(z + NZ - 1, NZ)
    sibling = (i, z * 4 + xh * 2 + 1 - c)
    partner = ((1 - xl) * NY + y, j)
    y_right, y_left = (xl * NY + yr, j), (xl * NY + yl, j)
    z_right, z_left = (i, zr * 4 + xh * 2 + c), (i, zl * 4 + xh * 2 + c)

    planes = (z, zl, zr)

    def in_plane(dx, to_y, core, n=0):
        to = lax.rem(x + dx, 4)
        return (lax.rem(to, 2) * NY + to_y, planes[n] * 4 + (to // 2) * 2 + core)

    inputs = [
        pltpu.make_async_copy(src, dst, in_sem.at[n])
        for n, (src, dst) in enumerate(((tokens_ref, tokens), (gain_ref, gain), (bias_ref, bias)))
    ]
    for load in inputs:
        load.start()
    barrier = pltpu.get_barrier_semaphore()

    with scope("greet"):
        for dx, dy in OFFSETS:
            to_y = lax.rem(y + dy, NY)
            for core, n in ((c, 1), (c, 2), (c, 0), (1 - c, 1), (1 - c, 2), (1 - c, 0)):
                if n == 0 and dx == 0 and dy == 0 and core is c:
                    continue
                pl.semaphore_signal(
                    barrier, inc=1, device_id=in_plane(dx, to_y, core, n), device_id_type=MESH
                )

    loads = [
        pltpu.make_async_copy(w, w_qkv.at[:, n * HEAD : (n + 1) * HEAD], win_sem.at[n])
        for n, w in enumerate((w_query, w_key, w_value))
    ]
    loads.append(pltpu.make_async_copy(w_inner, w_in, win_sem.at[3]))
    loads.append(pltpu.make_async_copy(w_attn, w_at, win_sem.at[4]))
    loads.append(pltpu.make_async_copy(w_outer, w_out, win_sem.at[5]))
    for load in loads:
        load.start()
    for load in inputs:
        load.wait()

    with scope("norm"):
        normed = (normalize(tokens[...].astype(F32)) * gain[...]).astype(BF16)
        for p in range(NX * NY):
            nsend[p] = normed[:, p * depth : (p + 1) * depth]
        lane = i * 2 + xh
        nrecv[0, c, lane] = nsend[i]
    with scope("barrier"):
        pl.semaphore_wait(barrier, 12 * NX * NY - 1)

    n_lane = 2 * NX * NY
    with scope("plane"):
        for n in (0, 1, 2):
            for dx, dy in OFFSETS:
                if n == 0 and dx == 0 and dy == 0:
                    continue
                target = in_plane(dx, lax.rem(y + dy, NY), c, n)
                send(nsend.at[target[0]], nrecv.at[n, c, lane], n_send, n_recv.at[n], target)

    def share_plane(n):
        wait_bytes(nrecv.at[n, 0, pl.ds(0, n_lane - (n == 0))], n_recv.at[n])
        send(nrecv.at[n, c], nrecv.at[n, c], m_send, m_recv.at[n], sibling)

    def build(n, k):
        wait_bytes(nrecv.at[n, 0], m_recv.at[n])
        for q in range(NX * NY):
            p = q % NX * NY + q // NX
            for s in range(4):
                at = q * tile + s * rows
                stage[n, at : at + rows, :] = nrecv[n, s % 2, p * 2 + s // 2].astype(F32)
        xg[k] = stage[n].astype(BF16).reshape(xg.shape[1:])

    cols = (pl.ds(0, half), pl.ds(half, half))
    piece = 8 * rows
    parts = (pl.ds(0, piece), pl.ds(piece, piece))

    def pass_on(src, dst, n, target):
        send(
            xg.at[src, c, parts[n]], xg.at[dst, c, parts[n]], r_send, r_recv.at[dst, n], target
        )

    def ring(k, n):
        if k == 0:
            for n in (0, 1, 2):
                share_plane(n)
                if n == 0:
                    build(0, 0)
            return
        if k == 4:
            for n in (0, 1):
                wait_bytes(xg.at[4, 0, parts[n]], r_recv.at[4, n])
            send(xg.at[4, c], xg.at[4, c], s_send, s_recv.at[4], sibling)
            return
        if k not in (1, 7):
            wait_bytes(xg.at[k, 0, parts[n]], r_recv.at[k, n])
        if k not in (3, 5) or (k, n) in ((5, 0), (3, 1)):
            pass_on(k, k - 1 if k > 4 else k + 1, n, z_right if k > 4 else z_left)
        if n == 1 and k not in (1, 7):
            send(xg.at[k, c], xg.at[k, c], s_send, s_recv.at[k], sibling)

    def project(g, k):
        low, high, _ = GROUPS[g]
        if k not in (0, 1, 7) and g == 0:
            wait_bytes(xg.at[k, 0], s_recv.at[k])
        w = w_qkv[...] if g == 0 else w_in[:, low - 384 : high - 384]
        pf[k, :, :, :, low:high] = jnp.dot(
            xg[k].reshape(8 * tile, depth), w, preferred_element_type=F32
        ).reshape(NY, NX, tile, high - low)

    def finish(g, k, total):
        low, high, _ = GROUPS[g]
        if g == 0:
            qkv[PLACE[k]] = total.astype(BF16)
            return
        low, high = low - 384, high - 384
        shift = jnp.concatenate([bias[h : h + 1] for h in range(low // HEAD, high // HEAD)], axis=1)
        inner = total + shift
        activ = 0.5 * inner * (1.0 + lax.erf(inner * math.sqrt(0.5)))
        ag[k, me, :, low:high] = activ.astype(BF16)
        if k in GATHER_AT_ONCE:
            gather_all(ag, (k,), k)
        elif k in Y_FIRST and k not in GATHER_IN_TWO:
            block = ag.at[k, me]
            send(block, block, gy_send, gr_recv.at[k], y_right)
            send(block, block, gy_send, gl_recv.at[k], y_left)
        else:
            send(ag.at[k, me], ag.at[k, me], gx_send, gx_recv.at[k], partner)

    def slices(g, k):
        width = GROUPS[g][1] - GROUPS[g][0]
        cut = (width // HEAD + k % 2) // 2 * HEAD
        return cut, pl.ds(0, cut), pl.ds(cut, width - cut)

    def start_ring(g, k, far):
        asend, arecv, _, _, _, _, a_send, ar, al, _, _, _ = groups[g][:12]
        _, right, left = slices(g, k)
        asend[k] = far.astype(BF16)
        at = (k,) + (slice(None),) * (len(asend.shape) - 2)
        send(asend.at[at + (right,)], arecv.at[at + (right,)], a_send, ar.at[k], y_right)
        send(asend.at[at + (left,)], arecv.at[at + (left,)], a_send, al.at[k], y_left)

    def relay(g, k, block):
        _, arecv, brs, brr, bls, blr, _, ar, al, b_send, br, bl = groups[g][:12]
        cut, right, left = slices(g, k)
        at = (k,) + (slice(None),) * (len(arecv.shape) - 2)
        value = block(yr)
        wait_bytes(arecv.at[at + (right,)], ar.at[k])
        brs[k] = jnp.concatenate(
            [value[..., :cut] + arecv[at + (slice(0, cut),)].astype(F32), value[..., cut:]], axis=-1
        ).astype(BF16)
        send(brs.at[k], brr.at[k], b_send, br.at[k], y_right)
        value = block(yl)
        wait_bytes(arecv.at[at + (left,)], al.at[k])
        bls[k] = jnp.concatenate(
            [value[..., :cut], value[..., cut:] + arecv[at + (slice(cut, None),)].astype(F32)], axis=-1
        ).astype(BF16)
        send(bls.at[k], blr.at[k], b_send, bl.at[k], y_left)

    def arrived(g, k, block):
        _, _, _, brr, _, blr, _, _, _, _, br, bl = groups[g][:12]
        wait_bytes(brr.at[k], br.at[k])
        wait_bytes(blr.at[k], bl.at[k])
        return block(y) + brr[k].astype(F32) + blr[k].astype(F32)

    def reduce_two(k, step):
        low, high, _ = GROUPS[1]
        dsend, drecv, d_send, d_recv = direct[1]
        sf, xsend, xrecv, x_send, x_recv = groups[1][12:]
        if step == 0:
            dsend[k] = pf[k, :, :, :, low:high].reshape(dsend.shape[1:]).astype(BF16)
            for n, to in enumerate((y2, yr, yl)):
                send(
                    dsend.at[k, pl.ds(to * NX, NX)], drecv.at[k, pl.ds(n * NX, NX)],
                    d_send, d_recv.at[k], (xl * NY + to, j),
                )
        elif step == 1:
            wait_bytes(drecv.at[k, pl.ds(0, 3 * NX)], d_recv.at[k])
            total = pf[k, y, :, :, low:high]
            for n in range(3):
                total = total + drecv[k, n * NX : (n + 1) * NX].astype(F32)
            xsend[k] = jnp.where(xl == 0, total[1], total[0]).astype(BF16)
            send(xsend.at[k], xrecv.at[k], x_send, x_recv.at[k], partner)
            sf[k] = jnp.where(xl == 0, total[0], total[1])
        elif step == 2:
            wait_bytes(xrecv.at[k], x_recv.at[k])
            finish(1, k, sf[k] + xrecv[k].astype(F32))

    def reduce_x_then_all(k, step):
        low, high, _ = GROUPS[0]
        dsend, drecv, d_send, d_recv = direct[0]
        sf, xsend, xrecv, x_send, x_recv = groups[0][12:]
        if step == 0:
            xsend[k] = pf[k, :, 1 - xl, :, low:high].astype(BF16)
            send(xsend.at[k], xrecv.at[k], x_send, x_recv.at[k], partner)
        elif step == 1:
            wait_bytes(xrecv.at[k], x_recv.at[k])
            sf[k] = pf[k, :, xl, :, low:high] + xrecv[k].astype(F32)
            dsend[k, :NY] = sf[k].astype(BF16)
            for n, to in enumerate((y2, yr, yl)):
                send(dsend.at[k, to], drecv.at[k, n], d_send, d_recv.at[k], (xl * NY + to, j))
        elif step == 2:
            wait_bytes(drecv.at[k, pl.ds(0, 3)], d_recv.at[k])
            total = sf[k, y]
            for n in range(3):
                total = total + drecv[k, n].astype(F32)
            finish(0, k, total)

    def reduce_all(g, k, step):
        low, high, _ = GROUPS[g]
        dsend, drecv, d_send, d_recv = direct[g]
        if step == 0:
            dsend[k] = pf[k, :, :, :, low:high].reshape(dsend.shape[1:]).astype(BF16)
            for n, (dx, dy) in enumerate(PEERS):
                to, target = peer(dx, dy)
                send(dsend.at[k, to], drecv.at[k, n], d_send, d_recv.at[k], target)
        elif step == 1:
            wait_bytes(drecv.at[k], d_recv.at[k])
            total = pf[k, y, xl, :, low:high]
            for n in range(len(PEERS)):
                total = total + drecv[k, n].astype(F32)
            finish(g, k, total)

    def reduce(g, k, step):
        if k in REDUCE_AT_ONCE[g]:
            return reduce_all(g, k, step)
        if g == 0 and k in X_THEN_ALL:
            return reduce_x_then_all(k, step)
        if g == 1 and k in REDUCE_IN_TWO:
            return reduce_two(k, step)
        low, high, first = GROUPS[g]
        sf, xsend, xrecv, x_send, x_recv = groups[g][12:]
        if first == "x":
            block = lambda at: sf[k, at]
            if step == 0:
                xsend[k] = pf[k, :, 1 - xl, :, low:high].astype(BF16)
                send(xsend.at[k], xrecv.at[k], x_send, x_recv.at[k], partner)
            elif step == 1:
                wait_bytes(xrecv.at[k], x_recv.at[k])
                sf[k] = pf[k, :, xl, :, low:high] + xrecv[k].astype(F32)
                start_ring(g, k, sf[k, y2])
            elif step == 2:
                relay(g, k, block)
            else:
                finish(g, k, arrived(g, k, block))
        else:
            block = lambda at: pf[k, at, :, :, low:high]
            if step == 0:
                start_ring(g, k, block(y2))
            elif step == 1:
                relay(g, k, block)
            elif step == 2:
                total = arrived(g, k, block)
                xsend[k] = jnp.where(xl == 0, total[1], total[0]).astype(BF16)
                send(xsend.at[k], xrecv.at[k], x_send, x_recv.at[k], partner)
                sf[k] = jnp.where(xl == 0, total[0], total[1])
            else:
                wait_bytes(xrecv.at[k], x_recv.at[k])
                finish(g, k, sf[k] + xrecv[k].astype(F32))

    def spread(g, at, k):
        pair = g.at[at + (pl.ds(y * NX, NX),)]
        wait_bytes(g.at[at + (0,)], gx_recv.at[k])
        send(pair, pair, h_send, hr_recv.at[k], (xl * NY + y2, j))
        send(pair, pair, gy_send, gr_recv.at[k], y_right)
        send(pair, pair, gy_send, gl_recv.at[k], y_left)

    def spread_done(g, at, k):
        for sem in (gr_recv, gl_recv, hr_recv):
            wait_bytes(g.at[at + (pl.ds(0, NX),)], sem.at[k])

    def peer(dx, dy):
        to_x, to_y = lax.rem(xl + dx, NX), lax.rem(y + dy, NY)
        return to_y * NX + to_x, (to_x * NY + to_y, j)

    def gather_all(g, at, n):
        own = g.at[at + (me,)]
        for dx, dy in PEERS:
            send(own, own, gd_send, gd_recv.at[n], peer(dx, dy)[1])

    def gather_y(k):
        if k in GATHER_IN_TWO:
            spread(ag, (k,), k)
            return
        if k in Y_FIRST:
            wait_bytes(ag.at[k, 0], gr_recv.at[k])
            block = ag.at[k, yl * NX + xl, :, cols[0]]
            send(block, block, h_send, hr_recv.at[k], y_right)
            wait_bytes(ag.at[k, 0], gl_recv.at[k])
            block = ag.at[k, yr * NX + xl, :, cols[1]]
            send(block, block, h_send, hl_recv.at[k], y_left)
            return
        wait_bytes(ag.at[k, 0], gx_recv.at[k])
        pair = ag.at[k, pl.ds(y * NX, NX)]
        send(pair, pair, gy_send, gr_recv.at[k], y_right)
        send(pair, pair, gy_send, gl_recv.at[k], y_left)

    def gather_far(k):
        if k in GATHER_IN_TWO:
            return
        if k in Y_FIRST:
            wait_bytes(ag.at[k, 0, :, cols[0]], hr_recv.at[k])
            wait_bytes(ag.at[k, 0, :, cols[1]], hl_recv.at[k])
            for n in range(NY):
                block = ag.at[k, n * NX + xl]
                send(block, block, gx_send, gx_recv.at[k], partner)
            return
        wait_bytes(ag.at[k, pl.ds(0, NX)], gr_recv.at[k])
        block = ag.at[k, yl * NX]
        send(block, block, h_send, hr_recv.at[k], y_right)
        wait_bytes(ag.at[k, pl.ds(0, NX)], gl_recv.at[k])
        block = ag.at[k, yr * NX + 1]
        send(block, block, h_send, hl_recv.at[k], y_left)

    def gather_done(k):
        if k in GATHER_AT_ONCE:
            wait_bytes(ag.at[k, pl.ds(0, NX * NY - 1)], gd_recv.at[k])
            return
        if k in GATHER_IN_TWO:
            spread_done(ag, (k,), k)
            return
        if k in Y_FIRST:
            wait_bytes(ag.at[k, pl.ds(0, NY)], gx_recv.at[k])
            return
        wait_bytes(ag.at[k, 0], hr_recv.at[k])
        wait_bytes(ag.at[k, 0], hl_recv.at[k])

    def attend():
        query = qkv[:, :, :HEAD].reshape(8 * tile, HEAD)
        key = qkv[:, :, HEAD : 2 * HEAD].reshape(8 * tile, HEAD)
        value = qkv[:, :, 2 * HEAD :].reshape(8 * tile, HEAD)
        query_norm = normalize(query.astype(F32)).astype(BF16)
        key_norm = normalize(key.astype(F32)).astype(BF16)
        scores = lax.dot_general(
            query_norm, key_norm, (((1,), (1,)), ((), ())), preferred_element_type=F32
        )
        scores = scores * (temper[0] * (1.0 / math.sqrt(HEAD)))
        weight = jnp.exp(scores - jnp.max(scores, axis=-1, keepdims=True))
        probs = (weight / jnp.sum(weight, axis=-1, keepdims=True)).astype(BF16)
        mg[me] = jnp.dot(probs, value, preferred_element_type=F32).astype(BF16)
        for n, group in enumerate(MIX):
            own = mg.at[me, pl.ds(PLACE[group[0]] * tile, len(group) * tile)]
            for dx, dy in PEERS:
                send(own, own, gd_send, gd_recv.at[8 + n], peer(dx, dy)[1])

    mixed_here = []

    def mixed_done(k):
        for n, group in enumerate(MIX):
            if k in group and n not in mixed_here:
                wait_bytes(mg.at[pl.ds(0, len(PEERS)), pl.ds(0, len(group) * tile)], gd_recv.at[8 + n])
                mixed_here.append(n)

    def project_out(k):
        gather_done(k)
        mixed_done(k)
        hidden = ag[k].reshape(8 * tile, depth)
        at = tile * PLACE[k]
        mixed = mg[:, at : at + tile, :].reshape(8 * tile, HEAD)
        total = jnp.dot(hidden, w_out[...], preferred_element_type=F32)
        total = total + jnp.dot(mixed, w_at[...], preferred_element_type=F32)
        og[k] = total.reshape(og.shape[1:])
        esend[k] = og[k, 1 - c].astype(BF16)
        send(esend.at[k], erecv.at[k], e_send, e_recv.at[k], sibling)

    def combined(k):
        wait_bytes(erecv.at[k], e_recv.at[k])
        return og[k, c] + erecv[k].astype(F32)

    def reduce_out(k, n):
        span = slice(n * half, (n + 1) * half)
        if k not in summed:
            wait_bytes(erecv.at[k], e_recv.at[k])
            summed.append(k)
        value = og[k, c, :, span] + erecv[k, :, span].astype(F32)
        if k in (2, 6) or (k, n) in ((3, 0), (5, 1)):
            wait_bytes(rrecv.at[k, :, cols[n]], z_recv.at[k, n])
            value = value + rrecv[k, :, span].astype(F32)
        rsend[k, :, span] = value.astype(BF16)
        right = k < 4 or (k == 4 and n == 0)
        to = k - 1 if right else k + 1
        send(
            rsend.at[k, :, cols[n]], rrecv.at[to, :, cols[n]], z_send, z_recv.at[to, n],
            z_right if right else z_left,
        )

    def scatter_out(n, total):
        for q in range(4):
            for s in range(4):
                at = q * tile + s * rows
                fsend[n, q * 4 + s] = total[at : at + rows].astype(BF16)
        slot = i * 2 + xh
        for dx in (2, 1, 3, 0):
            to = lax.rem(x + dx, 4)
            for yy in (0, 1):
                for core in (c, 1 - c):
                    src = (yy * NX + lax.rem(to, 2)) * 4 + (to // 2) * 2 + core
                    target = in_plane(dx, 2 * c + yy, core, n)
                    if n or dx or core is not c:
                        send(fsend.at[n, src], frecv.at[n, slot], f_send, f_recv.at[n], target)
                        continue
                    own = y == 2 * c + yy

                    @pl.when(own)
                    def _():
                        frecv[n, slot] = fsend[n, src]

                    @pl.when(jnp.logical_not(own))
                    def _():
                        send(fsend.at[n, src], frecv.at[n, slot], f_send, f_recv.at[n], target)

    def finish_out(k):
        total = combined(k)
        for n in (0, 1):
            wait_bytes(rrecv.at[k, :, cols[n]], z_recv.at[k, n])
        scatter_out(2 if k == 1 else 1, total + rrecv[k].astype(F32))

    summed = []

    def step(op, n, k):
        if op == "r":
            ring(k, n)
        elif op == "b":
            build(1 if k == 1 else 2, k)
        elif op == "p":
            project(n, k)
        elif op in "qm":
            reduce("qm".index(op), k, n)
        elif op == "y":
            gather_y(k)
        elif op == "f":
            gather_far(k)
        elif op == "w":
            for load in loads[4:] if n else loads[:4]:
                load.wait()
        elif op == "a":
            attend()
        elif op == "o":
            project_out(k)
        elif op == "s" and k in (1, 7):
            finish_out(k)
        elif op == "s":
            reduce_out(k, n)

    for word in SCHEDULE:
        name, k = word.split(".")
        with scope(f"{name}#k={k}"):
            step(name[0], int(name[1:] or 0), int(k))

    with scope("last"):
        scatter_out(0, combined(0))
    with scope("final"):
        mine = c == y // 2

        @pl.when(mine)
        def _():
            wait_bytes(frecv.at[0, pl.ds(0, n_lane - 1)], f_recv.at[0])
            wait_bytes(frecv.at[0, pl.ds(0, n_lane - 1)], f_send)

        @pl.when(jnp.logical_not(mine))
        def _():
            wait_bytes(frecv.at[0], f_recv.at[0])
            wait_bytes(frecv.at[0], f_send)

        for n in (1, 2):
            wait_bytes(frecv.at[n], f_recv.at[n])
            wait_bytes(frecv.at[n], f_send)

    for p in range(NX * NY):
        span = slice(p * depth, (p + 1) * depth)
        total = tokens[:, span].astype(F32)
        for n in range(3):
            total = total + frecv[n, 2 * p].astype(F32) + frecv[n, 2 * p + 1].astype(F32)
        out[:, span] = total.astype(BF16)

    wait_bytes(nrecv.at[0, 0, pl.ds(0, n_lane - 1)], n_send)
    wait_bytes(nrecv.at[0], n_send)
    wait_bytes(nrecv.at[:, 0], m_send)
    wait_bytes(xg.at[pl.ds(0, 5), 0], r_send)
    wait_bytes(xg.at[pl.ds(0, 5), 0], s_send)
    for g, scratch in enumerate(groups):
        once, two = len(REDUCE_AT_ONCE[g]), len((X_THEN_ALL, REDUCE_IN_TWO)[g])
        asend, _, brs, _, bls, _, a_send, _, _, b_send, _, _, _, xsend, _, x_send, _ = scratch
        for ref, sem in ((asend, a_send), (brs, b_send), (bls, b_send)):
            wait_bytes(ref.at[pl.ds(0, NZ - once - two)], sem)
        wait_bytes(xsend.at[pl.ds(0, NZ - once)], x_send)
        if once:
            wait_bytes(direct[g][1].at[pl.ds(0, once)], direct[g][2])
        if two:
            wait_bytes(direct[g][1].at[pl.ds(0, two), pl.ds(0, 3 + 3 * g)], direct[g][2])
    at_once = [k for k in GATHER_AT_ONCE if k < 8]
    late = len(Y_FIRST)
    n = NZ - len(at_once) - late
    for count, blocks in ((n, (1, 4, 2)), (late, (4, 2, 1))):
        for width, sem in zip(blocks, (gx_send, gy_send, h_send)):
            if count:
                wait_bytes(ag.at[pl.ds(0, count), pl.ds(0, width)], sem)
    if at_once:
        wait_bytes(ag.at[pl.ds(0, len(at_once)), pl.ds(0, NX * NY - 1)], gd_send)
    wait_bytes(mg.at[pl.ds(0, NX * NY - 1)], gd_send)
    wait_bytes(esend, e_send)
    wait_bytes(rsend.at[pl.ds(0, 5)], z_send)


def group_scratch(low, high, first, tile):
    dma = pltpu.SemaphoreType.DMA
    width = high - low
    ring = (NZ, tile, width) if first == "x" else (NZ, NX, tile, width)
    swap = (NZ, NY, tile, width) if first == "x" else (NZ, tile, width)
    return tuple(pltpu.VMEM(ring, BF16) for _ in range(6)) + (
        dma, dma((8,)), dma((8,)), dma, dma((8,)), dma((8,)),
        pltpu.VMEM(swap, F32), pltpu.VMEM(swap, BF16), pltpu.VMEM(swap, BF16), dma, dma((8,)),
    )


def per_device(
    tokens, norm_gain, w_query, w_key, w_value, w_inner, bias_inner, w_attn_out, w_outer, temper
):
    rows, width = tokens.shape
    depth = w_query.shape[0]
    hidden = w_inner.shape[1]
    wide = 3 * HEAD
    tile = 4 * rows
    vmem = pl.BlockSpec(memory_space=pltpu.VMEM)
    smem = pl.BlockSpec(memory_space=pltpu.SMEM)
    hbm = pl.BlockSpec(memory_space=pl.ANY)
    dma = pltpu.SemaphoreType.DMA
    return pl.pallas_call(
        block_kernel,
        out_shape=jax.ShapeDtypeStruct((rows, width), BF16),
        in_specs=[hbm, hbm, hbm, smem] + [hbm] * 6,
        out_specs=vmem,
        scratch_shapes=[
            pltpu.VMEM((rows, width), BF16),
            pltpu.VMEM((1, width), F32),
            pltpu.VMEM((hidden // HEAD, HEAD), F32),
            pltpu.VMEM((depth, wide), BF16),
            pltpu.VMEM((depth, hidden), BF16),
            pltpu.VMEM((HEAD, depth), BF16),
            pltpu.VMEM((hidden, depth), BF16),
            pltpu.VMEM((8, rows, depth), BF16),
            pltpu.VMEM((3, 2, 16, rows, depth), BF16),
            pltpu.VMEM((3, 8 * tile, depth), F32),
            pltpu.VMEM((NZ, 2, 4 * tile, depth), BF16),
            pltpu.VMEM((NZ, NY, NX, tile, wide + hidden), F32),
            tuple(group_scratch(*g, tile) for g in GROUPS),
            tuple(
                (
                    pltpu.VMEM((NZ, NX * NY, tile, high - low), BF16),
                    pltpu.VMEM((NZ, len(PEERS), tile, high - low), BF16),
                    dma, dma((8,)),
                )
                for low, high, _ in GROUPS
            ),
            pltpu.VMEM((NZ, tile, wide), BF16),
            pltpu.VMEM((NZ, NX * NY, tile, hidden), BF16),
            pltpu.VMEM((NX * NY, 8 * tile, HEAD), BF16),
            pltpu.VMEM((NZ, 2, 4 * tile, depth), F32),
            pltpu.VMEM((NZ, 4 * tile, depth), BF16),
            pltpu.VMEM((NZ, 4 * tile, depth), BF16),
            pltpu.VMEM((NZ, 4 * tile, depth), BF16),
            pltpu.VMEM((NZ + 1, 4 * tile, depth), BF16),
            pltpu.VMEM((3, 16, rows, depth), BF16),
            pltpu.VMEM((3, 16, rows, depth), BF16),
            dma((3,)), dma((6,)), dma, dma((3,)), dma, dma((3,)), dma, dma((8, 2)), dma, dma((8,)),
            dma, dma((13,)),
            dma, dma((9,)), dma, dma((9,)), dma((9,)), dma, dma((9,)), dma((9,)),
            dma, dma((8,)), dma, dma((9, 2)), dma, dma((3,)),
        ],
        compiler_params=pltpu.CompilerParams(
            collective_id=0, has_side_effects=True, vmem_limit_bytes=60 * 1024 * 1024
        ),
        name="encoder_block",
    )(
        tokens, norm_gain.reshape(1, -1), bias_inner.reshape(-1, HEAD), temper,
        w_query, w_key, w_value, w_inner, w_attn_out, w_outer,
    )


def solution(mesh):
    return jax.shard_map(
        per_device,
        mesh=mesh,
        in_specs=(
            P(("dp", "mp"), None),
            P(),
            P("dp", "mp"),
            P("dp", "mp"),
            P("dp", "mp"),
            P("dp", "mp"),
            P("mp"),
            P("mp", "dp"),
            P("mp", "dp"),
            P("mp"),
        ),
        out_specs=P(("dp", "mp"), None),
        check_vma=False,
    )
```

```python
import functools
import math

import jax
import jax.numpy as jnp
from jax import lax
from jax.experimental import pallas as pl
from jax.experimental.pallas import tpu as pltpu
from jax.sharding import PartitionSpec as P

HEAD = 128
NX, NY, NZ = 2, 4, 8
MESH = pl.DeviceIdType.MESH
F32, BF16 = jnp.float32, jnp.bfloat16
GROUPS = ((0, 384, "x"), (384, 1152, "y"))
REDUCE_AT_ONCE = ((1,), (4, 5))
REDUCE_IN_TWO = (0,)
GATHER_AT_ONCE = (4, 7)
GATHER_IN_TWO = (2, 3)
Y_FIRST = (1, 5, 6)
X_THEN_ALL = (2, 3, 4)
MIX = ((4,), (3, 5), (2, 6), (1, 7), (0,))
PLACE = {k: n for n, k in enumerate(sum(MIX, ()))}
PEERS = tuple((dx, dy) for dy in (2, 1, 3, 0) for dx in (1, 0) if dx or dy)
SCHEDULE = (
    "r.0", "w0.0", "p0.0", "b.1", "q0.0", "r0.1", "b.7", "r0.7", "p0.1", "p1.0",
    "r1.7", "q0.1", "r1.1", "p0.7", "p1.7", "m0.0", "p1.1", "q0.7", "r0.6", "m0.1",
    "q1.0", "r0.2", "r1.6", "m0.7", "r1.2", "p0.6", "p1.6", "m0.6", "p0.2", "m1.1",
    "q0.2", "q1.7", "r0.3", "p1.2", "m0.2", "q2.0", "m1.0", "q0.6", "r0.5", "r1.5",
    "r1.3", "m1.6", "p0.5", "p0.3", "q0.5", "p1.3", "m0.3", "q0.3", "p1.5", "m0.5",
    "r.4", "q1.2", "p0.4", "q1.6", "m1.3", "q1.1", "q1.5", "p1.4", "q0.4", "m0.4",
    "q2.2", "m1.2", "m2.6", "q2.5", "m2.3", "q1.3", "m1.5", "m2.1", "q2.6", "q1.4",
    "q2.7", "m1.7", "m2.0", "m2.2", "q3.0", "m3.6", "m3.3", "y.5", "q2.3", "m1.4",
    "q3.7", "q2.4", "q3.5", "q3.6", "a.0", "h0.4", "m3.1", "y.6", "m2.7", "m3.2",
    "h1.4", "y.3", "f.5", "h2.4", "y.0", "y.2", "w1.0", "o.4", "f.6", "s1.4",
    "s0.4", "h4.4", "y.1", "o.5", "h3.4", "o.3", "s0.5", "m3.7", "s1.3", "s1.5",
    "s0.3", "o.6", "f.1", "o.2", "s0.6", "f.0", "s1.2", "s1.6", "s0.2", "o.7",
    "o.1", "o.0", "s0.7", "s0.1",
)
OFFSETS = sorted(
    ((dx, dy) for dx in range(4) for dy in range(NY)),
    key=lambda o: -(min(o[0], 4 - o[0]) + min(o[1], NY - o[1])),
)

scope = jax.named_scope


def normalize(values):
    center = values - jnp.mean(values, axis=-1, keepdims=True)
    spread = jnp.mean(center * center, axis=-1, keepdims=True)
    return center * lax.rsqrt(spread + 1e-06)


def wait_bytes(ref, sem):
    pltpu.make_async_copy(ref, ref, sem).wait()


def send(src, dst, send_sem, recv_sem, target):
    pltpu.make_async_remote_copy(
        src_ref=src, dst_ref=dst, send_sem=send_sem, recv_sem=recv_sem,
        device_id=target, device_id_type=MESH,
    ).start()


def block_kernel(
    tokens_ref, gain_ref, bias_ref, temper, w_query, w_key, w_value, w_inner, w_attn, w_outer,
    out,
    tokens, gain, bias, w_qkv, w_in, w_at, w_out, nsend, nrecv, stage, xg, pf, groups,
    direct, qkv, ag, mg, og, esend, erecv, rsend, rrecv, fsend, frecv,
    in_sem, win_sem, n_send, n_recv, m_send, m_recv, r_send, r_recv, s_send, s_recv,
    gd_send, gd_recv, gx_send, gx_recv, gy_send, gr_recv, gl_recv, h_send, hr_recv, hl_recv,
    e_send, e_recv, z_send, z_recv, f_send, f_recv,
):
    rows, depth = nsend.shape[1:]
    tile = 4 * rows
    half = depth // 2
    i, j = lax.axis_index("dp"), lax.axis_index("mp")
    xl, y = i // NY, lax.rem(i, NY)
    z, xh, c = j // 4, lax.rem(j // 2, 2), lax.rem(j, 2)
    x, me = xh * 2 + xl, y * NX + xl
    yr, yl, y2 = lax.rem(y + 1, NY), lax.rem(y + NY - 1, NY), lax.rem(y + 2, NY)
    zr, zl = lax.rem(z + 1, NZ), lax.rem(z + NZ - 1, NZ)
    sibling = (i, z * 4 + xh * 2 + 1 - c)
    partner = ((1 - xl) * NY + y, j)
    y_right, y_left = (xl * NY + yr, j), (xl * NY + yl, j)
    z_right, z_left = (i, zr * 4 + xh * 2 + c), (i, zl * 4 + xh * 2 + c)

    planes = (z, zl, zr)

    def in_plane(dx, to_y, core, n=0):
        to = lax.rem(x + dx, 4)
        return (lax.rem(to, 2) * NY + to_y, planes[n] * 4 + (to // 2) * 2 + core)

    inputs = [
        pltpu.make_async_copy(src, dst, in_sem.at[n])
        for n, (src, dst) in enumerate(((tokens_ref, tokens), (gain_ref, gain), (bias_ref, bias)))
    ]
    for load in inputs:
        load.start()
    barrier = pltpu.get_barrier_semaphore()

    with scope("greet"):
        for dx, dy in OFFSETS:
            to_y = lax.rem(y + dy, NY)
            for core, n in ((c, 1), (c, 2), (c, 0), (1 - c, 1), (1 - c, 2), (1 - c, 0)):
                if n == 0 and dx == 0 and dy == 0 and core is c:
                    continue
                pl.semaphore_signal(
                    barrier, inc=1, device_id=in_plane(dx, to_y, core, n), device_id_type=MESH
                )

    loads = [
        pltpu.make_async_copy(w, w_qkv.at[:, n * HEAD : (n + 1) * HEAD], win_sem.at[n])
        for n, w in enumerate((w_query, w_key, w_value))
    ]
    loads.append(pltpu.make_async_copy(w_inner, w_in, win_sem.at[3]))
    loads.append(pltpu.make_async_copy(w_attn, w_at, win_sem.at[4]))
    loads.append(pltpu.make_async_copy(w_outer, w_out, win_sem.at[5]))
    for load in loads:
        load.start()
    for load in inputs:
        load.wait()

    with scope("norm"):
        normed = (normalize(tokens[...].astype(F32)) * gain[...]).astype(BF16)
        for p in range(NX * NY):
            nsend[p] = normed[:, p * depth : (p + 1) * depth]
        lane = i * 2 + xh
        nrecv[0, c, lane] = nsend[i]
    with scope("barrier"):
        pl.semaphore_wait(barrier, 12 * NX * NY - 1)

    n_lane = 2 * NX * NY
    with scope("plane"):
        for n in (0, 1, 2):
            for dx, dy in OFFSETS:
                if n == 0 and dx == 0 and dy == 0:
                    continue
                target = in_plane(dx, lax.rem(y + dy, NY), c, n)
                send(nsend.at[target[0]], nrecv.at[n, c, lane], n_send, n_recv.at[n], target)

    def share_plane(n):
        wait_bytes(nrecv.at[n, 0, pl.ds(0, n_lane - (n == 0))], n_recv.at[n])
        send(nrecv.at[n, c], nrecv.at[n, c], m_send, m_recv.at[n], sibling)

    def build(n, k):
        wait_bytes(nrecv.at[n, 0], m_recv.at[n])
        for q in range(NX * NY):
            p = q % NX * NY + q // NX
            for s in range(4):
                at = q * tile + s * rows
                stage[n, at : at + rows, :] = nrecv[n, s % 2, p * 2 + s // 2].astype(F32)
        xg[k] = stage[n].astype(BF16).reshape(xg.shape[1:])

    cols = (pl.ds(0, half), pl.ds(half, half))
    piece = 8 * rows
    parts = (pl.ds(0, piece), pl.ds(piece, piece))

    def pass_on(src, dst, n, target):
        send(
            xg.at[src, c, parts[n]], xg.at[dst, c, parts[n]], r_send, r_recv.at[dst, n], target
        )

    def ring(k, n):
        if k == 0:
            for n in (0, 1, 2):
                share_plane(n)
                if n == 0:
                    build(0, 0)
            return
        if k == 4:
            for n in (0, 1):
                wait_bytes(xg.at[4, 0, parts[n]], r_recv.at[4, n])
            send(xg.at[4, c], xg.at[4, c], s_send, s_recv.at[4], sibling)
            return
        if k not in (1, 7):
            wait_bytes(xg.at[k, 0, parts[n]], r_recv.at[k, n])
        if k not in (3, 5) or (k, n) in ((5, 0), (3, 1)):
            pass_on(k, k - 1 if k > 4 else k + 1, n, z_right if k > 4 else z_left)
        if n == 1 and k not in (1, 7):
            send(xg.at[k, c], xg.at[k, c], s_send, s_recv.at[k], sibling)

    def project(g, k):
        low, high, _ = GROUPS[g]
        if k not in (0, 1, 7) and g == 0:
            wait_bytes(xg.at[k, 0], s_recv.at[k])
        w = w_qkv[...] if g == 0 else w_in[:, low - 384 : high - 384]
        pf[k, :, :, :, low:high] = jnp.dot(
            xg[k].reshape(8 * tile, depth), w, preferred_element_type=F32
        ).reshape(NY, NX, tile, high - low)

    def finish(g, k, total):
        low, high, _ = GROUPS[g]
        if g == 0:
            qkv[PLACE[k]] = total.astype(BF16)
            return
        low, high = low - 384, high - 384
        shift = jnp.concatenate([bias[h : h + 1] for h in range(low // HEAD, high // HEAD)], axis=1)
        inner = total + shift
        activ = 0.5 * inner * (1.0 + lax.erf(inner * math.sqrt(0.5)))
        ag[k, me, :, low:high] = activ.astype(BF16)
        if k in GATHER_AT_ONCE:
            gather_all(ag, (k,), k)
        elif k in Y_FIRST and k not in GATHER_IN_TWO:
            block = ag.at[k, me]
            send(block, block, gy_send, gr_recv.at[k], y_right)
            send(block, block, gy_send, gl_recv.at[k], y_left)
        else:
            send(ag.at[k, me], ag.at[k, me], gx_send, gx_recv.at[k], partner)

    def slices(g, k):
        width = GROUPS[g][1] - GROUPS[g][0]
        cut = (width // HEAD + k % 2) // 2 * HEAD
        return cut, pl.ds(0, cut), pl.ds(cut, width - cut)

    def start_ring(g, k, far):
        asend, arecv, _, _, _, _, a_send, ar, al, _, _, _ = groups[g][:12]
        _, right, left = slices(g, k)
        asend[k] = far.astype(BF16)
        at = (k,) + (slice(None),) * (len(asend.shape) - 2)
        send(asend.at[at + (right,)], arecv.at[at + (right,)], a_send, ar.at[k], y_right)
        send(asend.at[at + (left,)], arecv.at[at + (left,)], a_send, al.at[k], y_left)

    def relay(g, k, block):
        _, arecv, brs, brr, bls, blr, _, ar, al, b_send, br, bl = groups[g][:12]
        cut, right, left = slices(g, k)
        at = (k,) + (slice(None),) * (len(arecv.shape) - 2)
        value = block(yr)
        wait_bytes(arecv.at[at + (right,)], ar.at[k])
        brs[k] = jnp.concatenate(
            [value[..., :cut] + arecv[at + (slice(0, cut),)].astype(F32), value[..., cut:]], axis=-1
        ).astype(BF16)
        send(brs.at[k], brr.at[k], b_send, br.at[k], y_right)
        value = block(yl)
        wait_bytes(arecv.at[at + (left,)], al.at[k])
        bls[k] = jnp.concatenate(
            [value[..., :cut], value[..., cut:] + arecv[at + (slice(cut, None),)].astype(F32)], axis=-1
        ).astype(BF16)
        send(bls.at[k], blr.at[k], b_send, bl.at[k], y_left)

    def arrived(g, k, block):
        _, _, _, brr, _, blr, _, _, _, _, br, bl = groups[g][:12]
        wait_bytes(brr.at[k], br.at[k])
        wait_bytes(blr.at[k], bl.at[k])
        return block(y) + brr[k].astype(F32) + blr[k].astype(F32)

    def reduce_two(k, step):
        low, high, _ = GROUPS[1]
        dsend, drecv, d_send, d_recv = direct[1]
        sf, xsend, xrecv, x_send, x_recv = groups[1][12:]
        if step == 0:
            dsend[k] = pf[k, :, :, :, low:high].reshape(dsend.shape[1:]).astype(BF16)
            for n, to in enumerate((y2, yr, yl)):
                send(
                    dsend.at[k, pl.ds(to * NX, NX)], drecv.at[k, pl.ds(n * NX, NX)],
                    d_send, d_recv.at[k], (xl * NY + to, j),
                )
        elif step == 1:
            wait_bytes(drecv.at[k, pl.ds(0, 3 * NX)], d_recv.at[k])
            total = pf[k, y, :, :, low:high]
            for n in range(3):
                total = total + drecv[k, n * NX : (n + 1) * NX].astype(F32)
            xsend[k] = jnp.where(xl == 0, total[1], total[0]).astype(BF16)
            send(xsend.at[k], xrecv.at[k], x_send, x_recv.at[k], partner)
            sf[k] = jnp.where(xl == 0, total[0], total[1])
        elif step == 2:
            wait_bytes(xrecv.at[k], x_recv.at[k])
            finish(1, k, sf[k] + xrecv[k].astype(F32))

    def reduce_x_then_all(k, step):
        low, high, _ = GROUPS[0]
        dsend, drecv, d_send, d_recv = direct[0]
        sf, xsend, xrecv, x_send, x_recv = groups[0][12:]
        if step == 0:
            xsend[k] = pf[k, :, 1 - xl, :, low:high].astype(BF16)
            send(xsend.at[k], xrecv.at[k], x_send, x_recv.at[k], partner)
        elif step == 1:
            wait_bytes(xrecv.at[k], x_recv.at[k])
            sf[k] = pf[k, :, xl, :, low:high] + xrecv[k].astype(F32)
            dsend[k, :NY] = sf[k].astype(BF16)
            for n, to in enumerate((y2, yr, yl)):
                send(dsend.at[k, to], drecv.at[k, n], d_send, d_recv.at[k], (xl * NY + to, j))
        elif step == 2:
            wait_bytes(drecv.at[k, pl.ds(0, 3)], d_recv.at[k])
            total = sf[k, y]
            for n in range(3):
                total = total + drecv[k, n].astype(F32)
            finish(0, k, total)

    def reduce_all(g, k, step):
        low, high, _ = GROUPS[g]
        dsend, drecv, d_send, d_recv = direct[g]
        if step == 0:
            dsend[k] = pf[k, :, :, :, low:high].reshape(dsend.shape[1:]).astype(BF16)
            for n, (dx, dy) in enumerate(PEERS):
                to, target = peer(dx, dy)
                send(dsend.at[k, to], drecv.at[k, n], d_send, d_recv.at[k], target)
        elif step == 1:
            wait_bytes(drecv.at[k], d_recv.at[k])
            total = pf[k, y, xl, :, low:high]
            for n in range(len(PEERS)):
                total = total + drecv[k, n].astype(F32)
            finish(g, k, total)

    def reduce(g, k, step):
        if k in REDUCE_AT_ONCE[g]:
            return reduce_all(g, k, step)
        if g == 0 and k in X_THEN_ALL:
            return reduce_x_then_all(k, step)
        if g == 1 and k in REDUCE_IN_TWO:
            return reduce_two(k, step)
        low, high, first = GROUPS[g]
        sf, xsend, xrecv, x_send, x_recv = groups[g][12:]
        if first == "x":
            block = lambda at: sf[k, at]
            if step == 0:
                xsend[k] = pf[k, :, 1 - xl, :, low:high].astype(BF16)
                send(xsend.at[k], xrecv.at[k], x_send, x_recv.at[k], partner)
            elif step == 1:
                wait_bytes(xrecv.at[k], x_recv.at[k])
                sf[k] = pf[k, :, xl, :, low:high] + xrecv[k].astype(F32)
                start_ring(g, k, sf[k, y2])
            elif step == 2:
                relay(g, k, block)
            else:
                finish(g, k, arrived(g, k, block))
        else:
            block = lambda at: pf[k, at, :, :, low:high]
            if step == 0:
                start_ring(g, k, block(y2))
            elif step == 1:
                relay(g, k, block)
            elif step == 2:
                total = arrived(g, k, block)
                xsend[k] = jnp.where(xl == 0, total[1], total[0]).astype(BF16)
                send(xsend.at[k], xrecv.at[k], x_send, x_recv.at[k], partner)
                sf[k] = jnp.where(xl == 0, total[0], total[1])
            else:
                wait_bytes(xrecv.at[k], x_recv.at[k])
                finish(g, k, sf[k] + xrecv[k].astype(F32))

    def spread(g, at, k):
        pair = g.at[at + (pl.ds(y * NX, NX),)]
        wait_bytes(g.at[at + (0,)], gx_recv.at[k])
        send(pair, pair, h_send, hr_recv.at[k], (xl * NY + y2, j))
        send(pair, pair, gy_send, gr_recv.at[k], y_right)
        send(pair, pair, gy_send, gl_recv.at[k], y_left)

    def spread_done(g, at, k):
        for sem in (gr_recv, gl_recv, hr_recv):
            wait_bytes(g.at[at + (pl.ds(0, NX),)], sem.at[k])

    def peer(dx, dy):
        to_x, to_y = lax.rem(xl + dx, NX), lax.rem(y + dy, NY)
        return to_y * NX + to_x, (to_x * NY + to_y, j)

    def gather_all(g, at, n):
        own = g.at[at + (me,)]
        for dx, dy in PEERS:
            send(own, own, gd_send, gd_recv.at[n], peer(dx, dy)[1])

    def gather_y(k):
        if k in GATHER_IN_TWO:
            spread(ag, (k,), k)
            return
        if k in Y_FIRST:
            wait_bytes(ag.at[k, 0], gr_recv.at[k])
            block = ag.at[k, yl * NX + xl, :, cols[0]]
            send(block, block, h_send, hr_recv.at[k], y_right)
            wait_bytes(ag.at[k, 0], gl_recv.at[k])
            block = ag.at[k, yr * NX + xl, :, cols[1]]
            send(block, block, h_send, hl_recv.at[k], y_left)
            return
        wait_bytes(ag.at[k, 0], gx_recv.at[k])
        pair = ag.at[k, pl.ds(y * NX, NX)]
        send(pair, pair, gy_send, gr_recv.at[k], y_right)
        send(pair, pair, gy_send, gl_recv.at[k], y_left)

    def gather_far(k):
        if k in GATHER_IN_TWO:
            return
        if k in Y_FIRST:
            wait_bytes(ag.at[k, 0, :, cols[0]], hr_recv.at[k])
            wait_bytes(ag.at[k, 0, :, cols[1]], hl_recv.at[k])
            for n in range(NY):
                block = ag.at[k, n * NX + xl]
                send(block, block, gx_send, gx_recv.at[k], partner)
            return
        wait_bytes(ag.at[k, pl.ds(0, NX)], gr_recv.at[k])
        block = ag.at[k, yl * NX]
        send(block, block, h_send, hr_recv.at[k], y_right)
        wait_bytes(ag.at[k, pl.ds(0, NX)], gl_recv.at[k])
        block = ag.at[k, yr * NX + 1]
        send(block, block, h_send, hl_recv.at[k], y_left)

    def gather_done(k):
        if k in GATHER_AT_ONCE:
            wait_bytes(ag.at[k, pl.ds(0, NX * NY - 1)], gd_recv.at[k])
            return
        if k in GATHER_IN_TWO:
            spread_done(ag, (k,), k)
            return
        if k in Y_FIRST:
            wait_bytes(ag.at[k, pl.ds(0, NY)], gx_recv.at[k])
            return
        wait_bytes(ag.at[k, 0], hr_recv.at[k])
        wait_bytes(ag.at[k, 0], hl_recv.at[k])

    def attend():
        query = qkv[:, :, :HEAD].reshape(8 * tile, HEAD)
        key = qkv[:, :, HEAD : 2 * HEAD].reshape(8 * tile, HEAD)
        value = qkv[:, :, 2 * HEAD :].reshape(8 * tile, HEAD)
        query_norm = normalize(query.astype(F32)).astype(BF16)
        key_norm = normalize(key.astype(F32)).astype(BF16)
        scores = lax.dot_general(
            query_norm, key_norm, (((1,), (1,)), ((), ())), preferred_element_type=F32
        )
        scores = scores * (temper[0] * (1.0 / math.sqrt(HEAD)))
        weight = jnp.exp(scores - jnp.max(scores, axis=-1, keepdims=True))
        probs = (weight / jnp.sum(weight, axis=-1, keepdims=True)).astype(BF16)
        mg[me] = jnp.dot(probs, value, preferred_element_type=F32).astype(BF16)

    def gather_mixed(n):
        own = mg.at[me, pl.ds(PLACE[MIX[n][0]] * tile, len(MIX[n]) * tile)]
        for dx, dy in PEERS:
            send(own, own, gd_send, gd_recv.at[8 + n], peer(dx, dy)[1])

    mixed_here = []

    def mixed_done(k):
        for n, group in enumerate(MIX):
            if k in group and n not in mixed_here:
                wait_bytes(mg.at[pl.ds(0, len(PEERS)), pl.ds(0, len(group) * tile)], gd_recv.at[8 + n])
                mixed_here.append(n)

    def project_out(k):
        gather_done(k)
        mixed_done(k)
        hidden = ag[k].reshape(8 * tile, depth)
        at = tile * PLACE[k]
        mixed = mg[:, at : at + tile, :].reshape(8 * tile, HEAD)
        total = jnp.dot(hidden, w_out[...], preferred_element_type=F32)
        total = total + jnp.dot(mixed, w_at[...], preferred_element_type=F32)
        og[k] = total.reshape(og.shape[1:])
        esend[k] = og[k, 1 - c].astype(BF16)
        send(esend.at[k], erecv.at[k], e_send, e_recv.at[k], sibling)

    def combined(k):
        wait_bytes(erecv.at[k], e_recv.at[k])
        return og[k, c] + erecv[k].astype(F32)

    def reduce_out(k, n):
        span = slice(n * half, (n + 1) * half)
        if k not in summed:
            wait_bytes(erecv.at[k], e_recv.at[k])
            summed.append(k)
        value = og[k, c, :, span] + erecv[k, :, span].astype(F32)
        if k in (2, 6) or (k, n) in ((3, 0), (5, 1)):
            wait_bytes(rrecv.at[k, :, cols[n]], z_recv.at[k, n])
            value = value + rrecv[k, :, span].astype(F32)
        rsend[k, :, span] = value.astype(BF16)
        right = k < 4 or (k == 4 and n == 0)
        to = k - 1 if right else k + 1
        send(
            rsend.at[k, :, cols[n]], rrecv.at[to, :, cols[n]], z_send, z_recv.at[to, n],
            z_right if right else z_left,
        )

    def scatter_out(n, total):
        for q in range(4):
            for s in range(4):
                at = q * tile + s * rows
                fsend[n, q * 4 + s] = total[at : at + rows].astype(BF16)
        slot = i * 2 + xh
        for dx in (2, 1, 3, 0):
            to = lax.rem(x + dx, 4)
            for yy in (0, 1):
                for core in (c, 1 - c):
                    src = (yy * NX + lax.rem(to, 2)) * 4 + (to // 2) * 2 + core
                    target = in_plane(dx, 2 * c + yy, core, n)
                    if n or dx or core is not c:
                        send(fsend.at[n, src], frecv.at[n, slot], f_send, f_recv.at[n], target)
                        continue
                    own = y == 2 * c + yy

                    @pl.when(own)
                    def _():
                        frecv[n, slot] = fsend[n, src]

                    @pl.when(jnp.logical_not(own))
                    def _():
                        send(fsend.at[n, src], frecv.at[n, slot], f_send, f_recv.at[n], target)

    def finish_out(k):
        total = combined(k)
        for n in (0, 1):
            wait_bytes(rrecv.at[k, :, cols[n]], z_recv.at[k, n])
        scatter_out(2 if k == 1 else 1, total + rrecv[k].astype(F32))

    summed = []

    def step(op, n, k):
        if op == "r":
            ring(k, n)
        elif op == "b":
            build(1 if k == 1 else 2, k)
        elif op == "p":
            project(n, k)
        elif op in "qm":
            reduce("qm".index(op), k, n)
        elif op == "y":
            gather_y(k)
        elif op == "f":
            gather_far(k)
        elif op == "w":
            for load in loads[4:] if n else loads[:4]:
                load.wait()
        elif op == "a":
            attend()
        elif op == "h":
            gather_mixed(n)
        elif op == "o":
            project_out(k)
        elif op == "s" and k in (1, 7):
            finish_out(k)
        elif op == "s":
            reduce_out(k, n)

    for word in SCHEDULE:
        name, k = word.split(".")
        with scope(f"{name}#k={k}"):
            step(name[0], int(name[1:] or 0), int(k))

    with scope("last"):
        scatter_out(0, combined(0))
    with scope("final"):
        mine = c == y // 2

        @pl.when(mine)
        def _():
            wait_bytes(frecv.at[0, pl.ds(0, n_lane - 1)], f_recv.at[0])
            wait_bytes(frecv.at[0, pl.ds(0, n_lane - 1)], f_send)

        @pl.when(jnp.logical_not(mine))
        def _():
            wait_bytes(frecv.at[0], f_recv.at[0])
            wait_bytes(frecv.at[0], f_send)

        for n in (1, 2):
            wait_bytes(frecv.at[n], f_recv.at[n])
            wait_bytes(frecv.at[n], f_send)

    for p in range(NX * NY):
        span = slice(p * depth, (p + 1) * depth)
        total = tokens[:, span].astype(F32)
        for n in range(3):
            total = total + frecv[n, 2 * p].astype(F32) + frecv[n, 2 * p + 1].astype(F32)
        out[:, span] = total.astype(BF16)

    wait_bytes(nrecv.at[0, 0, pl.ds(0, n_lane - 1)], n_send)
    wait_bytes(nrecv.at[0], n_send)
    wait_bytes(nrecv.at[:, 0], m_send)
    wait_bytes(xg.at[pl.ds(0, 5), 0], r_send)
    wait_bytes(xg.at[pl.ds(0, 5), 0], s_send)
    for g, scratch in enumerate(groups):
        once, two = len(REDUCE_AT_ONCE[g]), len((X_THEN_ALL, REDUCE_IN_TWO)[g])
        asend, _, brs, _, bls, _, a_send, _, _, b_send, _, _, _, xsend, _, x_send, _ = scratch
        for ref, sem in ((asend, a_send), (brs, b_send), (bls, b_send)):
            wait_bytes(ref.at[pl.ds(0, NZ - once - two)], sem)
        wait_bytes(xsend.at[pl.ds(0, NZ - once)], x_send)
        if once:
            wait_bytes(direct[g][1].at[pl.ds(0, once)], direct[g][2])
        if two:
            wait_bytes(direct[g][1].at[pl.ds(0, two), pl.ds(0, 3 + 3 * g)], direct[g][2])
    at_once = [k for k in GATHER_AT_ONCE if k < 8]
    late = len(Y_FIRST)
    n = NZ - len(at_once) - late
    for count, blocks in ((n, (1, 4, 2)), (late, (4, 2, 1))):
        for width, sem in zip(blocks, (gx_send, gy_send, h_send)):
            if count:
                wait_bytes(ag.at[pl.ds(0, count), pl.ds(0, width)], sem)
    if at_once:
        wait_bytes(ag.at[pl.ds(0, len(at_once)), pl.ds(0, NX * NY - 1)], gd_send)
    wait_bytes(mg.at[pl.ds(0, NX * NY - 1)], gd_send)
    wait_bytes(esend, e_send)
    wait_bytes(rsend.at[pl.ds(0, 5)], z_send)


def group_scratch(low, high, first, tile):
    dma = pltpu.SemaphoreType.DMA
    width = high - low
    ring = (NZ, tile, width) if first == "x" else (NZ, NX, tile, width)
    swap = (NZ, NY, tile, width) if first == "x" else (NZ, tile, width)
    return tuple(pltpu.VMEM(ring, BF16) for _ in range(6)) + (
        dma, dma((8,)), dma((8,)), dma, dma((8,)), dma((8,)),
        pltpu.VMEM(swap, F32), pltpu.VMEM(swap, BF16), pltpu.VMEM(swap, BF16), dma, dma((8,)),
    )


def per_device(
    tokens, norm_gain, w_query, w_key, w_value, w_inner, bias_inner, w_attn_out, w_outer, temper
):
    rows, width = tokens.shape
    depth = w_query.shape[0]
    hidden = w_inner.shape[1]
    wide = 3 * HEAD
    tile = 4 * rows
    vmem = pl.BlockSpec(memory_space=pltpu.VMEM)
    smem = pl.BlockSpec(memory_space=pltpu.SMEM)
    hbm = pl.BlockSpec(memory_space=pl.ANY)
    dma = pltpu.SemaphoreType.DMA
    return pl.pallas_call(
        block_kernel,
        out_shape=pltpu.VMEM((rows, width), BF16),
        in_specs=[hbm, hbm, hbm, smem] + [hbm] * 6,
        out_specs=vmem,
        scratch_shapes=[
            pltpu.VMEM((rows, width), BF16),
            pltpu.VMEM((1, width), F32),
            pltpu.VMEM((hidden // HEAD, HEAD), F32),
            pltpu.VMEM((depth, wide), BF16),
            pltpu.VMEM((depth, hidden), BF16),
            pltpu.VMEM((HEAD, depth), BF16),
            pltpu.VMEM((hidden, depth), BF16),
            pltpu.VMEM((8, rows, depth), BF16),
            pltpu.VMEM((3, 2, 16, rows, depth), BF16),
            pltpu.VMEM((3, 8 * tile, depth), F32),
            pltpu.VMEM((NZ, 2, 4 * tile, depth), BF16),
            pltpu.VMEM((NZ, NY, NX, tile, wide + hidden), F32),
            tuple(group_scratch(*g, tile) for g in GROUPS),
            tuple(
                (
                    pltpu.VMEM((NZ, NX * NY, tile, high - low), BF16),
                    pltpu.VMEM((NZ, len(PEERS), tile, high - low), BF16),
                    dma, dma((8,)),
                )
                for low, high, _ in GROUPS
            ),
            pltpu.VMEM((NZ, tile, wide), BF16),
            pltpu.VMEM((NZ, NX * NY, tile, hidden), BF16),
            pltpu.VMEM((NX * NY, 8 * tile, HEAD), BF16),
            pltpu.VMEM((NZ, 2, 4 * tile, depth), F32),
            pltpu.VMEM((NZ, 4 * tile, depth), BF16),
            pltpu.VMEM((NZ, 4 * tile, depth), BF16),
            pltpu.VMEM((NZ, 4 * tile, depth), BF16),
            pltpu.VMEM((NZ + 1, 4 * tile, depth), BF16),
            pltpu.VMEM((3, 16, rows, depth), BF16),
            pltpu.VMEM((3, 16, rows, depth), BF16),
            dma((3,)), dma((6,)), dma, dma((3,)), dma, dma((3,)), dma, dma((8, 2)), dma, dma((8,)),
            dma, dma((13,)),
            dma, dma((9,)), dma, dma((9,)), dma((9,)), dma, dma((9,)), dma((9,)),
            dma, dma((8,)), dma, dma((9, 2)), dma, dma((3,)),
        ],
        compiler_params=pltpu.CompilerParams(
            collective_id=0, has_side_effects=True, vmem_limit_bytes=60 * 1024 * 1024
        ),
        name="encoder_block",
    )(
        tokens, norm_gain.reshape(1, -1), bias_inner.reshape(-1, HEAD), temper,
        w_query, w_key, w_value, w_inner, w_attn_out, w_outer,
    )


def solution(mesh):
    return jax.shard_map(
        per_device,
        mesh=mesh,
        in_specs=(
            P(("dp", "mp"), None),
            P(),
            P("dp", "mp"),
            P("dp", "mp"),
            P("dp", "mp"),
            P("dp", "mp"),
            P("mp"),
            P("mp", "dp"),
            P("mp", "dp"),
            P("mp"),
        ),
        out_specs=P(("dp", "mp"), None),
        check_vma=False,
    )
```

```python
import functools
import math

import jax
import jax.numpy as jnp
from jax import lax
from jax.experimental import pallas as pl
from jax.experimental.pallas import tpu as pltpu
from jax.sharding import PartitionSpec as P

HEAD = 128
NX, NY, NZ = 2, 4, 8
MESH = pl.DeviceIdType.MESH
F32, BF16 = jnp.float32, jnp.bfloat16
GROUPS = ((0, 384, "x"), (384, 1152, "y"))
REDUCE_AT_ONCE = ((1,), (4, 5, 7))
REDUCE_IN_TWO = (0, 2)
GATHER_AT_ONCE = (4,)
GATHER_IN_TWO = (2, 3)
Y_FIRST = (1, 6)
X_THEN_ALL = (2, 3, 4)
MIX = ((4,), (3, 5), (2, 6), (1, 7), (0,))
PLACE = {k: n for n, k in enumerate(sum(MIX, ()))}
PEERS = tuple((dx, dy) for dy in (2, 1, 3, 0) for dx in (1, 0) if dx or dy)
SCHEDULE = (
    "r.0", "w0.0", "b.1", "r0.1", "b.7", "r0.7", "r1.1", "p0.1", "q0.1", "r1.7",
    "p0.0", "p1.1", "p1.0", "m0.1", "p0.7", "m0.0", "p1.7", "q0.7", "r0.2", "r0.6",
    "m0.7", "q0.0", "r1.2", "r1.6", "m1.1", "p0.2", "p1.2", "m0.2", "q1.7", "q0.2",
    "p0.6", "p1.6", "r0.3", "r0.5", "m0.6", "r1.3", "q0.6", "r1.5", "p0.3", "p0.5",
    "q0.5", "p1.3", "m0.3", "p1.5", "q1.0", "m0.5", "r.4", "q0.3", "m1.6", "p0.4",
    "p1.4", "q1.5", "q0.4", "m0.4", "m1.3", "m2.6", "q1.6", "q2.0", "q1.1", "m1.5",
    "q1.4", "q2.7", "q2.5", "m1.0", "m2.1", "q1.3", "q1.2", "m2.3", "q2.6", "m1.2",
    "m3.6", "y.5", "m1.4", "q2.4", "q3.7", "q3.0", "q3.6", "q3.5", "q2.2", "q2.3",
    "m3.3", "a.0", "h0.4", "m2.2", "m1.7", "m3.1", "h1.4", "y.6", "m2.0", "f.5",
    "y.3", "y.1", "h2.4", "w1.0", "o.4", "y.2", "f.6", "h3.4", "s1.4", "s0.4",
    "y.7", "y.0", "o.5", "o.3", "s0.5", "s1.3", "h4.4", "s1.5", "s0.3", "o.6",
    "f.1", "o.2", "f.7", "s0.6", "s1.2", "s1.6", "f.0", "s0.2", "o.7", "o.1",
    "o.0", "s0.7", "s0.1",
)
OFFSETS = sorted(
    ((dx, dy) for dx in range(4) for dy in range(NY)),
    key=lambda o: -(min(o[0], 4 - o[0]) + min(o[1], NY - o[1])),
)

scope = jax.named_scope


def normalize(values):
    center = values - jnp.mean(values, axis=-1, keepdims=True)
    spread = jnp.mean(center * center, axis=-1, keepdims=True)
    return center * lax.rsqrt(spread + 1e-06)


def wait_bytes(ref, sem):
    pltpu.make_async_copy(ref, ref, sem).wait()


def send(src, dst, send_sem, recv_sem, target):
    pltpu.make_async_remote_copy(
        src_ref=src, dst_ref=dst, send_sem=send_sem, recv_sem=recv_sem,
        device_id=target, device_id_type=MESH,
    ).start()


def block_kernel(
    tokens_ref, gain_ref, bias_ref, temper, w_query, w_key, w_value, w_inner, w_attn, w_outer,
    out,
    tokens, gain, bias, w_qkv, w_in, w_at, w_out, nsend, nrecv, stage, xg, pf, groups,
    direct, qkv, ag, mg, og, esend, erecv, rsend, rrecv, fsend, frecv,
    in_sem, win_sem, n_send, n_recv, m_send, m_recv, r_send, r_recv, s_send, s_recv,
    gd_send, gd_recv, gx_send, gx_recv, gy_send, gr_recv, gl_recv, h_send, hr_recv, hl_recv,
    e_send, e_recv, z_send, z_recv, f_send, f_recv,
):
    rows, depth = nsend.shape[1:]
    tile = 4 * rows
    half = depth // 2
    i, j = lax.axis_index("dp"), lax.axis_index("mp")
    xl, y = i // NY, lax.rem(i, NY)
    z, xh, c = j // 4, lax.rem(j // 2, 2), lax.rem(j, 2)
    x, me = xh * 2 + xl, y * NX + xl
    yr, yl, y2 = lax.rem(y + 1, NY), lax.rem(y + NY - 1, NY), lax.rem(y + 2, NY)
    zr, zl = lax.rem(z + 1, NZ), lax.rem(z + NZ - 1, NZ)
    sibling = (i, z * 4 + xh * 2 + 1 - c)
    partner = ((1 - xl) * NY + y, j)
    y_right, y_left = (xl * NY + yr, j), (xl * NY + yl, j)
    z_right, z_left = (i, zr * 4 + xh * 2 + c), (i, zl * 4 + xh * 2 + c)

    planes = (z, zl, zr)

    def in_plane(dx, to_y, core, n=0):
        to = lax.rem(x + dx, 4)
        return (lax.rem(to, 2) * NY + to_y, planes[n] * 4 + (to // 2) * 2 + core)

    inputs = [
        pltpu.make_async_copy(src, dst, in_sem.at[n])
        for n, (src, dst) in enumerate(((tokens_ref, tokens), (gain_ref, gain), (bias_ref, bias)))
    ]
    for load in inputs:
        load.start()
    barrier = pltpu.get_barrier_semaphore()

    with scope("greet"):
        for dx, dy in OFFSETS:
            to_y = lax.rem(y + dy, NY)
            for core, n in ((c, 1), (c, 2), (c, 0), (1 - c, 1), (1 - c, 2), (1 - c, 0)):
                if n == 0 and dx == 0 and dy == 0 and core is c:
                    continue
                pl.semaphore_signal(
                    barrier, inc=1, device_id=in_plane(dx, to_y, core, n), device_id_type=MESH
                )

    loads = [
        pltpu.make_async_copy(w, w_qkv.at[:, n * HEAD : (n + 1) * HEAD], win_sem.at[n])
        for n, w in enumerate((w_query, w_key, w_value))
    ]
    loads.append(pltpu.make_async_copy(w_inner, w_in, win_sem.at[3]))
    loads.append(pltpu.make_async_copy(w_attn, w_at, win_sem.at[4]))
    loads.append(pltpu.make_async_copy(w_outer, w_out, win_sem.at[5]))
    for load in loads:
        load.start()
    for load in inputs:
        load.wait()

    with scope("norm"):
        normed = (normalize(tokens[...].astype(F32)) * gain[...]).astype(BF16)
        for p in range(NX * NY):
            nsend[p] = normed[:, p * depth : (p + 1) * depth]
        lane = i * 2 + xh
        nrecv[0, c, lane] = nsend[i]
    with scope("barrier"):
        pl.semaphore_wait(barrier, 12 * NX * NY - 1)

    n_lane = 2 * NX * NY
    with scope("plane"):
        for n in (0, 1, 2):
            for dx, dy in OFFSETS:
                if n == 0 and dx == 0 and dy == 0:
                    continue
                target = in_plane(dx, lax.rem(y + dy, NY), c, n)
                send(nsend.at[target[0]], nrecv.at[n, c, lane], n_send, n_recv.at[n], target)

    def share_plane(n):
        wait_bytes(nrecv.at[n, 0, pl.ds(0, n_lane - (n == 0))], n_recv.at[n])
        send(nrecv.at[n, c], nrecv.at[n, c], m_send, m_recv.at[n], sibling)

    def build(n, k):
        wait_bytes(nrecv.at[n, 0], m_recv.at[n])
        for q in range(NX * NY):
            p = q % NX * NY + q // NX
            for s in range(4):
                at = q * tile + s * rows
                stage[n, at : at + rows, :] = nrecv[n, s % 2, p * 2 + s // 2].astype(F32)
        xg[k] = stage[n].astype(BF16).reshape(xg.shape[1:])

    cols = (pl.ds(0, half), pl.ds(half, half))
    piece = 8 * rows
    parts = (pl.ds(0, piece), pl.ds(piece, piece))

    def pass_on(src, dst, n, target):
        send(
            xg.at[src, c, parts[n]], xg.at[dst, c, parts[n]], r_send, r_recv.at[dst, n], target
        )

    def ring(k, n):
        if k == 0:
            for n in (0, 1, 2):
                share_plane(n)
                if n == 0:
                    build(0, 0)
            return
        if k == 4:
            for n in (0, 1):
                wait_bytes(xg.at[4, 0, parts[n]], r_recv.at[4, n])
            send(xg.at[4, c], xg.at[4, c], s_send, s_recv.at[4], sibling)
            return
        if k not in (1, 7):
            wait_bytes(xg.at[k, 0, parts[n]], r_recv.at[k, n])
        if k not in (3, 5) or (k, n) in ((5, 0), (3, 1)):
            pass_on(k, k - 1 if k > 4 else k + 1, n, z_right if k > 4 else z_left)
        if n == 1 and k not in (1, 7):
            send(xg.at[k, c], xg.at[k, c], s_send, s_recv.at[k], sibling)

    def project(g, k):
        low, high, _ = GROUPS[g]
        if k not in (0, 1, 7) and g == 0:
            wait_bytes(xg.at[k, 0], s_recv.at[k])
        w = w_qkv[...] if g == 0 else w_in[:, low - 384 : high - 384]
        pf[k, :, :, :, low:high] = jnp.dot(
            xg[k].reshape(8 * tile, depth), w, preferred_element_type=F32
        ).reshape(NY, NX, tile, high - low)

    def finish(g, k, total):
        low, high, _ = GROUPS[g]
        if g == 0:
            qkv[PLACE[k]] = total.astype(BF16)
            return
        low, high = low - 384, high - 384
        shift = jnp.concatenate([bias[h : h + 1] for h in range(low // HEAD, high // HEAD)], axis=1)
        inner = total + shift
        activ = 0.5 * inner * (1.0 + lax.erf(inner * math.sqrt(0.5)))
        ag[k, me, :, low:high] = activ.astype(BF16)
        if k in GATHER_AT_ONCE:
            gather_all(ag, (k,), k)
        elif k in Y_FIRST and k not in GATHER_IN_TWO:
            block = ag.at[k, me]
            send(block, block, gy_send, gr_recv.at[k], y_right)
            send(block, block, gy_send, gl_recv.at[k], y_left)
        else:
            send(ag.at[k, me], ag.at[k, me], gx_send, gx_recv.at[k], partner)

    def slices(g, k):
        width = GROUPS[g][1] - GROUPS[g][0]
        cut = (width // HEAD + k % 2) // 2 * HEAD
        return cut, pl.ds(0, cut), pl.ds(cut, width - cut)

    def start_ring(g, k, far):
        asend, arecv, _, _, _, _, a_send, ar, al, _, _, _ = groups[g][:12]
        _, right, left = slices(g, k)
        asend[k] = far.astype(BF16)
        at = (k,) + (slice(None),) * (len(asend.shape) - 2)
        send(asend.at[at + (right,)], arecv.at[at + (right,)], a_send, ar.at[k], y_right)
        send(asend.at[at + (left,)], arecv.at[at + (left,)], a_send, al.at[k], y_left)

    def relay(g, k, block):
        _, arecv, brs, brr, bls, blr, _, ar, al, b_send, br, bl = groups[g][:12]
        cut, right, left = slices(g, k)
        at = (k,) + (slice(None),) * (len(arecv.shape) - 2)
        value = block(yr)
        wait_bytes(arecv.at[at + (right,)], ar.at[k])
        brs[k] = jnp.concatenate(
            [value[..., :cut] + arecv[at + (slice(0, cut),)].astype(F32), value[..., cut:]], axis=-1
        ).astype(BF16)
        send(brs.at[k], brr.at[k], b_send, br.at[k], y_right)
        value = block(yl)
        wait_bytes(arecv.at[at + (left,)], al.at[k])
        bls[k] = jnp.concatenate(
            [value[..., :cut], value[..., cut:] + arecv[at + (slice(cut, None),)].astype(F32)], axis=-1
        ).astype(BF16)
        send(bls.at[k], blr.at[k], b_send, bl.at[k], y_left)

    def arrived(g, k, block):
        _, _, _, brr, _, blr, _, _, _, _, br, bl = groups[g][:12]
        wait_bytes(brr.at[k], br.at[k])
        wait_bytes(blr.at[k], bl.at[k])
        return block(y) + brr[k].astype(F32) + blr[k].astype(F32)

    def reduce_two(k, step):
        low, high, _ = GROUPS[1]
        dsend, drecv, d_send, d_recv = direct[1]
        sf, xsend, xrecv, x_send, x_recv = groups[1][12:]
        if step == 0:
            dsend[k] = pf[k, :, :, :, low:high].reshape(dsend.shape[1:]).astype(BF16)
            for n, to in enumerate((y2, yr, yl)):
                send(
                    dsend.at[k, pl.ds(to * NX, NX)], drecv.at[k, pl.ds(n * NX, NX)],
                    d_send, d_recv.at[k], (xl * NY + to, j),
                )
        elif step == 1:
            wait_bytes(drecv.at[k, pl.ds(0, 3 * NX)], d_recv.at[k])
            total = pf[k, y, :, :, low:high]
            for n in range(3):
                total = total + drecv[k, n * NX : (n + 1) * NX].astype(F32)
            xsend[k] = jnp.where(xl == 0, total[1], total[0]).astype(BF16)
            send(xsend.at[k], xrecv.at[k], x_send, x_recv.at[k], partner)
            sf[k] = jnp.where(xl == 0, total[0], total[1])
        elif step == 2:
            wait_bytes(xrecv.at[k], x_recv.at[k])
            finish(1, k, sf[k] + xrecv[k].astype(F32))

    def reduce_x_then_all(k, step):
        low, high, _ = GROUPS[0]
        dsend, drecv, d_send, d_recv = direct[0]
        sf, xsend, xrecv, x_send, x_recv = groups[0][12:]
        if step == 0:
            xsend[k] = pf[k, :, 1 - xl, :, low:high].astype(BF16)
            send(xsend.at[k], xrecv.at[k], x_send, x_recv.at[k], partner)
        elif step == 1:
            wait_bytes(xrecv.at[k], x_recv.at[k])
            sf[k] = pf[k, :, xl, :, low:high] + xrecv[k].astype(F32)
            dsend[k, :NY] = sf[k].astype(BF16)
            for n, to in enumerate((y2, yr, yl)):
                send(dsend.at[k, to], drecv.at[k, n], d_send, d_recv.at[k], (xl * NY + to, j))
        elif step == 2:
            wait_bytes(drecv.at[k, pl.ds(0, 3)], d_recv.at[k])
            total = sf[k, y]
            for n in range(3):
                total = total + drecv[k, n].astype(F32)
            finish(0, k, total)

    def reduce_all(g, k, step):
        low, high, _ = GROUPS[g]
        dsend, drecv, d_send, d_recv = direct[g]
        if step == 0:
            dsend[k] = pf[k, :, :, :, low:high].reshape(dsend.shape[1:]).astype(BF16)
            for n, (dx, dy) in enumerate(PEERS):
                to, target = peer(dx, dy)
                send(dsend.at[k, to], drecv.at[k, n], d_send, d_recv.at[k], target)
        elif step == 1:
            wait_bytes(drecv.at[k], d_recv.at[k])
            total = pf[k, y, xl, :, low:high]
            for n in range(len(PEERS)):
                total = total + drecv[k, n].astype(F32)
            finish(g, k, total)

    def reduce(g, k, step):
        if k in REDUCE_AT_ONCE[g]:
            return reduce_all(g, k, step)
        if g == 0 and k in X_THEN_ALL:
            return reduce_x_then_all(k, step)
        if g == 1 and k in REDUCE_IN_TWO:
            return reduce_two(k, step)
        low, high, first = GROUPS[g]
        sf, xsend, xrecv, x_send, x_recv = groups[g][12:]
        if first == "x":
            block = lambda at: sf[k, at]
            if step == 0:
                xsend[k] = pf[k, :, 1 - xl, :, low:high].astype(BF16)
                send(xsend.at[k], xrecv.at[k], x_send, x_recv.at[k], partner)
            elif step == 1:
                wait_bytes(xrecv.at[k], x_recv.at[k])
                sf[k] = pf[k, :, xl, :, low:high] + xrecv[k].astype(F32)
                start_ring(g, k, sf[k, y2])
            elif step == 2:
                relay(g, k, block)
            else:
                finish(g, k, arrived(g, k, block))
        else:
            block = lambda at: pf[k, at, :, :, low:high]
            if step == 0:
                start_ring(g, k, block(y2))
            elif step == 1:
                relay(g, k, block)
            elif step == 2:
                total = arrived(g, k, block)
                xsend[k] = jnp.where(xl == 0, total[1], total[0]).astype(BF16)
                send(xsend.at[k], xrecv.at[k], x_send, x_recv.at[k], partner)
                sf[k] = jnp.where(xl == 0, total[0], total[1])
            else:
                wait_bytes(xrecv.at[k], x_recv.at[k])
                finish(g, k, sf[k] + xrecv[k].astype(F32))

    def spread(g, at, k):
        pair = g.at[at + (pl.ds(y * NX, NX),)]
        wait_bytes(g.at[at + (0,)], gx_recv.at[k])
        send(pair, pair, h_send, hr_recv.at[k], (xl * NY + y2, j))
        send(pair, pair, gy_send, gr_recv.at[k], y_right)
        send(pair, pair, gy_send, gl_recv.at[k], y_left)

    def spread_done(g, at, k):
        for sem in (gr_recv, gl_recv, hr_recv):
            wait_bytes(g.at[at + (pl.ds(0, NX),)], sem.at[k])

    def peer(dx, dy):
        to_x, to_y = lax.rem(xl + dx, NX), lax.rem(y + dy, NY)
        return to_y * NX + to_x, (to_x * NY + to_y, j)

    def gather_all(g, at, n):
        own = g.at[at + (me,)]
        for dx, dy in PEERS:
            send(own, own, gd_send, gd_recv.at[n], peer(dx, dy)[1])

    def gather_y(k):
        if k in GATHER_IN_TWO:
            spread(ag, (k,), k)
            return
        if k in Y_FIRST:
            wait_bytes(ag.at[k, 0], gr_recv.at[k])
            block = ag.at[k, yl * NX + xl, :, cols[0]]
            send(block, block, h_send, hr_recv.at[k], y_right)
            wait_bytes(ag.at[k, 0], gl_recv.at[k])
            block = ag.at[k, yr * NX + xl, :, cols[1]]
            send(block, block, h_send, hl_recv.at[k], y_left)
            return
        wait_bytes(ag.at[k, 0], gx_recv.at[k])
        pair = ag.at[k, pl.ds(y * NX, NX)]
        send(pair, pair, gy_send, gr_recv.at[k], y_right)
        send(pair, pair, gy_send, gl_recv.at[k], y_left)

    def gather_far(k):
        if k in GATHER_IN_TWO:
            return
        if k in Y_FIRST:
            wait_bytes(ag.at[k, 0, :, cols[0]], hr_recv.at[k])
            wait_bytes(ag.at[k, 0, :, cols[1]], hl_recv.at[k])
            for n in range(NY):
                block = ag.at[k, n * NX + xl]
                send(block, block, gx_send, gx_recv.at[k], partner)
            return
        wait_bytes(ag.at[k, pl.ds(0, NX)], gr_recv.at[k])
        block = ag.at[k, yl * NX]
        send(block, block, h_send, hr_recv.at[k], y_right)
        wait_bytes(ag.at[k, pl.ds(0, NX)], gl_recv.at[k])
        block = ag.at[k, yr * NX + 1]
        send(block, block, h_send, hl_recv.at[k], y_left)

    def gather_done(k):
        if k in GATHER_AT_ONCE:
            wait_bytes(ag.at[k, pl.ds(0, NX * NY - 1)], gd_recv.at[k])
            return
        if k in GATHER_IN_TWO:
            spread_done(ag, (k,), k)
            return
        if k in Y_FIRST:
            wait_bytes(ag.at[k, pl.ds(0, NY)], gx_recv.at[k])
            return
        wait_bytes(ag.at[k, 0], hr_recv.at[k])
        wait_bytes(ag.at[k, 0], hl_recv.at[k])

    def attend():
        query = qkv[:, :, :HEAD].reshape(8 * tile, HEAD)
        key = qkv[:, :, HEAD : 2 * HEAD].reshape(8 * tile, HEAD)
        value = qkv[:, :, 2 * HEAD :].reshape(8 * tile, HEAD)
        query_norm = normalize(query.astype(F32)).astype(BF16)
        key_norm = normalize(key.astype(F32)).astype(BF16)
        scores = lax.dot_general(
            query_norm, key_norm, (((1,), (1,)), ((), ())), preferred_element_type=F32
        )
        scores = scores * (temper[0] * (1.0 / math.sqrt(HEAD)))
        weight = jnp.exp(scores - jnp.max(scores, axis=-1, keepdims=True))
        probs = (weight / jnp.sum(weight, axis=-1, keepdims=True)).astype(BF16)
        mg[me] = jnp.dot(probs, value, preferred_element_type=F32).astype(BF16)

    def gather_mixed(n):
        own = mg.at[me, pl.ds(PLACE[MIX[n][0]] * tile, len(MIX[n]) * tile)]
        for dx, dy in PEERS:
            send(own, own, gd_send, gd_recv.at[8 + n], peer(dx, dy)[1])

    mixed_here = []

    def mixed_done(k):
        for n, group in enumerate(MIX):
            if k in group and n not in mixed_here:
                wait_bytes(mg.at[pl.ds(0, len(PEERS)), pl.ds(0, len(group) * tile)], gd_recv.at[8 + n])
                mixed_here.append(n)

    def project_out(k):
        gather_done(k)
        mixed_done(k)
        hidden = ag[k].reshape(8 * tile, depth)
        at = tile * PLACE[k]
        mixed = mg[:, at : at + tile, :].reshape(8 * tile, HEAD)
        total = jnp.dot(hidden, w_out[...], preferred_element_type=F32)
        total = total + jnp.dot(mixed, w_at[...], preferred_element_type=F32)
        og[k] = total.reshape(og.shape[1:])
        esend[k] = og[k, 1 - c].astype(BF16)
        send(esend.at[k], erecv.at[k], e_send, e_recv.at[k], sibling)

    def combined(k):
        wait_bytes(erecv.at[k], e_recv.at[k])
        return og[k, c] + erecv[k].astype(F32)

    def reduce_out(k, n):
        span = slice(n * half, (n + 1) * half)
        if k not in summed:
            wait_bytes(erecv.at[k], e_recv.at[k])
            summed.append(k)
        value = og[k, c, :, span] + erecv[k, :, span].astype(F32)
        if k in (2, 6) or (k, n) in ((3, 0), (5, 1)):
            wait_bytes(rrecv.at[k, :, cols[n]], z_recv.at[k, n])
            value = value + rrecv[k, :, span].astype(F32)
        rsend[k, :, span] = value.astype(BF16)
        right = k < 4 or (k == 4 and n == 0)
        to = k - 1 if right else k + 1
        send(
            rsend.at[k, :, cols[n]], rrecv.at[to, :, cols[n]], z_send, z_recv.at[to, n],
            z_right if right else z_left,
        )

    def scatter_out(n, total):
        for q in range(4):
            for s in range(4):
                at = q * tile + s * rows
                fsend[n, q * 4 + s] = total[at : at + rows].astype(BF16)
        slot = i * 2 + xh
        for dx in (2, 1, 3, 0):
            to = lax.rem(x + dx, 4)
            for yy in (0, 1):
                for core in (c, 1 - c):
                    src = (yy * NX + lax.rem(to, 2)) * 4 + (to // 2) * 2 + core
                    target = in_plane(dx, 2 * c + yy, core, n)
                    if n or dx or core is not c:
                        send(fsend.at[n, src], frecv.at[n, slot], f_send, f_recv.at[n], target)
                        continue
                    own = y == 2 * c + yy

                    @pl.when(own)
                    def _():
                        frecv[n, slot] = fsend[n, src]

                    @pl.when(jnp.logical_not(own))
                    def _():
                        send(fsend.at[n, src], frecv.at[n, slot], f_send, f_recv.at[n], target)

    def finish_out(k):
        total = combined(k)
        for n in (0, 1):
            wait_bytes(rrecv.at[k, :, cols[n]], z_recv.at[k, n])
        scatter_out(2 if k == 1 else 1, total + rrecv[k].astype(F32))

    summed = []

    def step(op, n, k):
        if op == "r":
            ring(k, n)
        elif op == "b":
            build(1 if k == 1 else 2, k)
        elif op == "p":
            project(n, k)
        elif op in "qm":
            reduce("qm".index(op), k, n)
        elif op == "y":
            gather_y(k)
        elif op == "f":
            gather_far(k)
        elif op == "w":
            for load in loads[4:] if n else loads[:4]:
                load.wait()
        elif op == "a":
            attend()
        elif op == "h":
            gather_mixed(n)
        elif op == "o":
            project_out(k)
        elif op == "s" and k in (1, 7):
            finish_out(k)
        elif op == "s":
            reduce_out(k, n)

    for word in SCHEDULE:
        name, k = word.split(".")
        with scope(f"{name}#k={k}"):
            step(name[0], int(name[1:] or 0), int(k))

    with scope("last"):
        scatter_out(0, combined(0))
    with scope("final"):
        mine = c == y // 2

        @pl.when(mine)
        def _():
            wait_bytes(frecv.at[0, pl.ds(0, n_lane - 1)], f_recv.at[0])
            wait_bytes(frecv.at[0, pl.ds(0, n_lane - 1)], f_send)

        @pl.when(jnp.logical_not(mine))
        def _():
            wait_bytes(frecv.at[0], f_recv.at[0])
            wait_bytes(frecv.at[0], f_send)

        for n in (1, 2):
            wait_bytes(frecv.at[n], f_recv.at[n])
            wait_bytes(frecv.at[n], f_send)

    for p in range(NX * NY):
        span = slice(p * depth, (p + 1) * depth)
        total = tokens[:, span].astype(F32)
        for n in range(3):
            total = total + frecv[n, 2 * p].astype(F32) + frecv[n, 2 * p + 1].astype(F32)
        out[:, span] = total.astype(BF16)

    wait_bytes(nrecv.at[0, 0, pl.ds(0, n_lane - 1)], n_send)
    wait_bytes(nrecv.at[0], n_send)
    wait_bytes(nrecv.at[:, 0], m_send)
    wait_bytes(xg.at[pl.ds(0, 5), 0], r_send)
    wait_bytes(xg.at[pl.ds(0, 5), 0], s_send)
    for g, scratch in enumerate(groups):
        once, two = len(REDUCE_AT_ONCE[g]), len((X_THEN_ALL, REDUCE_IN_TWO)[g])
        asend, _, brs, _, bls, _, a_send, _, _, b_send, _, _, _, xsend, _, x_send, _ = scratch
        for ref, sem in ((asend, a_send), (brs, b_send), (bls, b_send)):
            wait_bytes(ref.at[pl.ds(0, NZ - once - two)], sem)
        wait_bytes(xsend.at[pl.ds(0, NZ - once)], x_send)
        if once:
            wait_bytes(direct[g][1].at[pl.ds(0, once)], direct[g][2])
        if two:
            wait_bytes(direct[g][1].at[pl.ds(0, two), pl.ds(0, 3 + 3 * g)], direct[g][2])
    at_once = [k for k in GATHER_AT_ONCE if k < 8]
    late = len(Y_FIRST)
    n = NZ - len(at_once) - late
    for count, blocks in ((n, (1, 4, 2)), (late, (4, 2, 1))):
        for width, sem in zip(blocks, (gx_send, gy_send, h_send)):
            if count:
                wait_bytes(ag.at[pl.ds(0, count), pl.ds(0, width)], sem)
    if at_once:
        wait_bytes(ag.at[pl.ds(0, len(at_once)), pl.ds(0, NX * NY - 1)], gd_send)
    wait_bytes(mg.at[pl.ds(0, NX * NY - 1)], gd_send)
    wait_bytes(esend, e_send)
    wait_bytes(rsend.at[pl.ds(0, 5)], z_send)


def group_scratch(low, high, first, tile):
    dma = pltpu.SemaphoreType.DMA
    width = high - low
    ring = (NZ, tile, width) if first == "x" else (NZ, NX, tile, width)
    swap = (NZ, NY, tile, width) if first == "x" else (NZ, tile, width)
    return tuple(pltpu.VMEM(ring, BF16) for _ in range(6)) + (
        dma, dma((8,)), dma((8,)), dma, dma((8,)), dma((8,)),
        pltpu.VMEM(swap, F32), pltpu.VMEM(swap, BF16), pltpu.VMEM(swap, BF16), dma, dma((8,)),
    )


def per_device(
    tokens, norm_gain, w_query, w_key, w_value, w_inner, bias_inner, w_attn_out, w_outer, temper
):
    rows, width = tokens.shape
    depth = w_query.shape[0]
    hidden = w_inner.shape[1]
    wide = 3 * HEAD
    tile = 4 * rows
    vmem = pl.BlockSpec(memory_space=pltpu.VMEM)
    smem = pl.BlockSpec(memory_space=pltpu.SMEM)
    hbm = pl.BlockSpec(memory_space=pl.ANY)
    dma = pltpu.SemaphoreType.DMA
    return pl.pallas_call(
        block_kernel,
        out_shape=pltpu.VMEM((rows, width), BF16),
        in_specs=[hbm, hbm, hbm, smem] + [hbm] * 6,
        out_specs=vmem,
        scratch_shapes=[
            pltpu.VMEM((rows, width), BF16),
            pltpu.VMEM((1, width), F32),
            pltpu.VMEM((hidden // HEAD, HEAD), F32),
            pltpu.VMEM((depth, wide), BF16),
            pltpu.VMEM((depth, hidden), BF16),
            pltpu.VMEM((HEAD, depth), BF16),
            pltpu.VMEM((hidden, depth), BF16),
            pltpu.VMEM((8, rows, depth), BF16),
            pltpu.VMEM((3, 2, 16, rows, depth), BF16),
            pltpu.VMEM((3, 8 * tile, depth), F32),
            pltpu.VMEM((NZ, 2, 4 * tile, depth), BF16),
            pltpu.VMEM((NZ, NY, NX, tile, wide + hidden), F32),
            tuple(group_scratch(*g, tile) for g in GROUPS),
            tuple(
                (
                    pltpu.VMEM((NZ, NX * NY, tile, high - low), BF16),
                    pltpu.VMEM((NZ, len(PEERS), tile, high - low), BF16),
                    dma, dma((8,)),
                )
                for low, high, _ in GROUPS
            ),
            pltpu.VMEM((NZ, tile, wide), BF16),
            pltpu.VMEM((NZ, NX * NY, tile, hidden), BF16),
            pltpu.VMEM((NX * NY, 8 * tile, HEAD), BF16),
            pltpu.VMEM((NZ, 2, 4 * tile, depth), F32),
            pltpu.VMEM((NZ, 4 * tile, depth), BF16),
            pltpu.VMEM((NZ, 4 * tile, depth), BF16),
            pltpu.VMEM((NZ, 4 * tile, depth), BF16),
            pltpu.VMEM((NZ + 1, 4 * tile, depth), BF16),
            pltpu.VMEM((3, 16, rows, depth), BF16),
            pltpu.VMEM((3, 16, rows, depth), BF16),
            dma((3,)), dma((6,)), dma, dma((3,)), dma, dma((3,)), dma, dma((8, 2)), dma, dma((8,)),
            dma, dma((13,)),
            dma, dma((9,)), dma, dma((9,)), dma((9,)), dma, dma((9,)), dma((9,)),
            dma, dma((8,)), dma, dma((9, 2)), dma, dma((3,)),
        ],
        compiler_params=pltpu.CompilerParams(
            collective_id=0, has_side_effects=True, vmem_limit_bytes=60 * 1024 * 1024
        ),
        name="encoder_block",
    )(
        tokens, norm_gain.reshape(1, -1), bias_inner.reshape(-1, HEAD), temper,
        w_query, w_key, w_value, w_inner, w_attn_out, w_outer,
    )


def solution(mesh):
    return jax.shard_map(
        per_device,
        mesh=mesh,
        in_specs=(
            P(("dp", "mp"), None),
            P(),
            P("dp", "mp"),
            P("dp", "mp"),
            P("dp", "mp"),
            P("dp", "mp"),
            P("mp"),
            P("mp", "dp"),
            P("mp", "dp"),
            P("mp"),
        ),
        out_specs=P(("dp", "mp"), None),
        check_vma=False,
    )
```
